256 devices in a mesh: dp: 8 (over y, core), expert: 8 (over z), ffn: 4 (over x).
Axes of the slice: x: 4, y: 4, z: 8, core: 2. Of those that a mesh axis runs over, the one named last changes fastest.
Arguments:
- tokens: bfloat16 [1024, 4096], P('expert'), may hold values from -6 to 6
- expert_ids: int32 [1024, 2], P('expert'), may hold values from 0 to 7, all different within a row; in each aligned block of 128 rows (0 to 127, 128 to 255, ...) at most 64 rows name the same one
- route_weight: float32 [1024, 2], P('expert'), may hold values from 0.05 to 1
- cotangent: bfloat16 [1024, 4096], P('expert'), may hold values from -40 to 40
- w_gate: bfloat16 [8, 7168, 4096], P('expert', ('dp', 'ffn')), may hold values from -0.09375 to 0.09375
- w_up: bfloat16 [8, 7168, 4096], P('expert', ('dp', 'ffn')), may hold values from -0.09375 to 0.09375
- w_down: bfloat16 [8, 7168, 4096], P('expert', ('dp', 'ffn')), may hold values from -0.0625 to 0.0625
Outputs:
- layer_out: bfloat16 [1024, 4096], P('expert', ('dp', 'ffn'))
- ascent_gate: bfloat16 [8, 7168, 4096], P('expert', ('dp', 'ffn'))
- ascent_up: bfloat16 [8, 7168, 4096], P('expert', ('dp', 'ffn'))
- ascent_down: bfloat16 [8, 7168, 4096], P('expert', ('dp', 'ffn'))
The draws below stay inside these ranges and needn't reach their ends.
Inputs may be any that keep to these rules, and one draw needn't show every extreme that they name: `expert_ids`: each row names two different experts. Among the rows of one aligned block of 128 no expert is named more than 64 times; in every draw some block names some expert exactly 64 times.
All inputs are finite; a program needn't handle non-finite values.
Results may differ from the reference program's by a relative error of at most 0.017.
Values may be sent and summed in bfloat16 or wider, within the bound.
A program may use at most 128 MiB of HBM per device.

```python
import math
import jax
import jax.numpy as jnp
import numpy as np
from jax import lax

D = 4096
FF = 7168
TOP = 2
TOK_DEV = 128
EXPERTS = 8
CAP = 64
TOKENS = 1024
SLOTS = 512
GROUPS = 32


def draw_cotangent(key, part):
    base_key, row_key, col_key = jax.random.split(key, 3)
    row_count = TOKENS
    position = jnp.arange(row_count, dtype=jnp.float32) / row_count
    row_scale = jnp.exp(jax.random.uniform(row_key, (row_count, 1), jnp.float32, 0.0, 2.3))
    col_scale = jnp.exp(jax.random.uniform(col_key, (1, D), jnp.float32, 0.0, 1.1))
    values = jnp.clip(jax.random.normal(base_key, (row_count, D), jnp.float32), -4.0, 4.0) * (3.0 ** position)[:, None]
    return jnp.clip(values * row_scale * col_scale * 0.3, -40.0, 40.0).astype(jnp.bfloat16)


def shard_levels(own_key, shape, cuts, least, high):
    factor_of = 1.0
    for axis_at, shards_of in cuts:
        heights = jax.random.uniform(jax.random.fold_in(jax.random.fold_in(own_key, 6), axis_at), (shards_of,), jnp.float32, least / len(cuts), high / len(cuts))
        factor_of = factor_of * jnp.repeat(jnp.exp(heights), shape[axis_at] // shards_of).reshape((-1,) + (1,) * (len(shape) - 1 - axis_at))
    return factor_of


def deal_out(stream_key, own, number, rows, amount, top, bound, slope):
    ranking = jax.random.permutation(stream_key, amount)
    crowded, ordinary = shares(amount, rows * top, bound, slope, True), shares(amount, rows * top, bound, slope, False)
    places = jnp.arange(amount)

    def named(sizes, rotation):
        used = int((sizes > 0).sum())
        fixed = max(1, used // 4)
        shifted = fixed + (places - fixed + rotation * (used - fixed)) % max(1, amount - fixed)
        return jnp.zeros((amount,), jnp.int32).at[ranking[jnp.where(places < fixed, places, shifted)]].set(jnp.asarray(sizes, jnp.int32))

    sizes = jnp.where(number % 4 == 0, named(crowded, number // 4), named(ordinary, number - number // 4 - 1))
    mixed = jax.random.permutation(jax.random.fold_in(own, 3), amount)
    source_of, taker = mixed[0:amount // 2 * 2:2], mixed[1:amount // 2 * 2:2]
    slack = jnp.minimum(sizes[source_of] - 1, bound - sizes[taker]) // 2
    slack = jnp.where((source_of == ranking[0]) | (taker == ranking[0]) | (sizes[taker] == 0), 0, jnp.maximum(slack, 0))
    shifted = jax.random.randint(jax.random.fold_in(own, 4), (amount // 2,), 0, 1 << 20) % (slack + 1)
    sizes = sizes.at[source_of].add(-shifted).at[taker].add(shifted)
    members = jnp.searchsorted(jnp.cumsum(sizes), jnp.arange(rows * top), side="right").astype(jnp.int32)
    grid = members.reshape(top, rows).T
    grid = grid[jax.random.permutation(jax.random.fold_in(own, 1), rows)]
    rotation = jax.random.randint(jax.random.fold_in(own, 2), (rows, 1), 0, top)
    return jnp.take_along_axis(grid, (jnp.arange(top)[None, :] + rotation) % top, axis=1)


def shares(number_of, total, limit, lean, full):
    weights = [(1 << 20) // math.isqrt(grade ** lean) + 1 for grade in range(1, number_of + 1)]
    largest = limit if full else min(limit, max(-(-total // number_of), total * weights[0] // sum(weights)))
    least = 1 if total - largest >= number_of - 1 else 0
    counts, spare = [largest] + [least] * (number_of - 1), total - largest - least * (number_of - 1)
    while spare > 0:
        movable = [i for i in range(1, number_of) if counts[i] < largest] or [i for i in range(1, number_of) if counts[i] < limit]
        mass, budget = sum([weights[i] for i in movable]), spare
        for i in movable:
            more = min(limit - counts[i], max(1, budget * weights[i] // mass), spare)
            counts[i] = counts[i] + more
            spare = spare - more
    return np.array(counts)


def bell_draw(own_key, extent, width, most, cuts=(), held_as=jnp.bfloat16):
    entries = jax.random.normal(own_key, extent, jnp.float32) * width
    if len(cuts) > 0:
        entries = shard_levels(own_key, extent, cuts, -0.22, 0.18) * entries
    return jnp.clip(entries, min=-most, max=most).astype(held_as)


def setup_inputs(seed: int = 0) -> dict:
    key_of = jax.random.split(jax.random.key(seed), 8)
    tokens = bell_draw(key_of[0], (TOKENS, D), 1.0, 6.0, ((0, 8),))
    expert_ids_keys = jax.random.split(jax.random.fold_in(key_of[1], 1), TOKENS // TOK_DEV)
    expert_ids_turns = jax.random.permutation(jax.random.fold_in(key_of[1], 3), TOKENS // TOK_DEV)
    expert_ids = jax.vmap(lambda own, number: deal_out(jax.random.fold_in(key_of[1], 2), own, number, TOK_DEV, EXPERTS, TOP, CAP, 2))(expert_ids_keys, expert_ids_turns).reshape((TOKENS, TOP))
    route_weight = jnp.clip(0.05 + 0.95 * jax.random.uniform(key_of[2], (TOKENS, TOP), jnp.float32) ** shard_levels(key_of[2], (TOKENS, TOP), ((0, 8),), -0.2, 0.2), 0.05, 1.0)
    cotangent = draw_cotangent(jax.random.fold_in(key_of[7], 71), 0)
    w_gate = bell_draw(key_of[4], (EXPERTS, FF, D), D ** -0.5, 0.09375, ((0, 8), (1, 32)))
    w_up = bell_draw(key_of[5], (EXPERTS, FF, D), D ** -0.5, 0.09375, ((0, 8), (1, 32)))
    w_down = bell_draw(key_of[6], (EXPERTS, FF, D), FF ** -0.5, 0.0625, ((0, 8), (1, 32)))
    return {"tokens": tokens, "expert_ids": expert_ids, "route_weight": route_weight, "cotangent": cotangent, "w_gate": w_gate, "w_up": w_up, "w_down": w_down}


def silu_parts(pre_act):
    sigmoid_value = jax.nn.sigmoid(pre_act)
    return (pre_act * sigmoid_value, sigmoid_value * (1.0 + pre_act * (1.0 - sigmoid_value)))

def against_rows(left_rows, right_rows):
    return lax.dot_general(left_rows.astype(jnp.float32), right_rows.astype(jnp.float32), (((0,), (0,)), ((), ())))

def across_width(left_rows, weight):
    return lax.dot_general(left_rows.astype(jnp.float32), weight.astype(jnp.float32), (((1,), (1,)), ((), ())))

def reference(tokens, expert_ids, route_weight, cotangent, w_gate, w_up, w_down):
    block_count = TOKENS // TOK_DEV
    route_ids = expert_ids.reshape(block_count, TOK_DEV, 2)
    chosen = route_ids[:, :, :, None] == jnp.arange(EXPERTS, dtype=jnp.int32)
    per_token = lax.optimization_barrier(jnp.sum(chosen.astype(jnp.int32), axis=2)).astype(jnp.int32)
    earlier = (jnp.cumsum(per_token, axis=1) - per_token).astype(jnp.int32)
    position = lax.optimization_barrier(jnp.sum(jnp.where(chosen, earlier[:, :, None, :], 0), axis=3)).astype(jnp.int32)
    block_start = (jnp.arange(block_count, dtype=jnp.int32) * CAP)[:, None, None]
    flat_slot = (route_ids * SLOTS + block_start + position).reshape(-1).astype(jnp.int32)
    scaled = (route_weight[:, :, None] * cotangent.astype(jnp.float32)[:, None, :]).astype(jnp.bfloat16)
    token_table = jnp.zeros((EXPERTS * SLOTS, D), jnp.bfloat16).at[flat_slot].set(jnp.repeat(tokens, 2, axis=0))
    grad_table = jnp.zeros((EXPERTS * SLOTS, D), jnp.bfloat16).at[flat_slot].set(scaled.reshape(TOKENS * 2, D))
    group_width = FF // GROUPS

    def one_expert(operands):
        slot_rows, slot_grads, gate_weight, up_weight, down_weight = operands
        pre_gate = across_width(slot_rows, gate_weight)
        pre_up = across_width(slot_rows, up_weight)
        activated, derivative = silu_parts(pre_gate)
        hidden = (activated * pre_up).astype(jnp.bfloat16)

        def add_group(running, part_index):
            start = (part_index * group_width).astype(jnp.int32)
            hidden_part = lax.dynamic_slice_in_dim(hidden, start, group_width, 1)
            weight_part = lax.dynamic_slice_in_dim(down_weight, start, group_width, 0)
            product = jnp.dot(hidden_part.astype(jnp.float32), weight_part.astype(jnp.float32))
            rounded = lax.optimization_barrier(product.astype(jnp.bfloat16))
            return (running + rounded.astype(jnp.float32), None)
        summed, _ = lax.scan(add_group, jnp.zeros((SLOTS, D), jnp.float32), jnp.arange(GROUPS, dtype=jnp.int32))
        grad_down = against_rows(hidden, slot_grads)
        grad_hidden = across_width(slot_grads, down_weight)
        delta_gate = (grad_hidden * pre_up * derivative).astype(jnp.bfloat16)
        delta_up = (grad_hidden * activated).astype(jnp.bfloat16)
        return (summed.astype(jnp.bfloat16), against_rows(delta_gate, slot_rows), against_rows(delta_up, slot_rows), grad_down)
    slot_out, grads_gate, grads_up, grads_down = lax.map(one_expert, (token_table.reshape(EXPERTS, SLOTS, D), grad_table.reshape(EXPERTS, SLOTS, D), w_gate, w_up, w_down))
    picked = slot_out.reshape(EXPERTS * SLOTS, D)[flat_slot].astype(jnp.float32).reshape(TOKENS, 2, D)
    layer_out = lax.optimization_barrier(jnp.sum(route_weight[:, :, None] * picked, axis=1)).astype(jnp.bfloat16)
    sum_squares = jnp.sum(grads_gate * grads_gate) + jnp.sum(grads_up * grads_up) + jnp.sum(grads_down * grads_down)
    inv_rms = lax.rsqrt(sum_squares / (3.0 * EXPERTS * FF * D) + 1e-06)
    return (layer_out, (grads_gate * inv_rms).astype(jnp.bfloat16), (grads_up * inv_rms).astype(jnp.bfloat16), (grads_down * inv_rms).astype(jnp.bfloat16))
```

```python
import jax
import jax.numpy as jnp
from jax import lax
from jax.sharding import Mesh
from jax.sharding import PartitionSpec as P

FF = 7168
DP_FFN = ("dp_0", "dp_1", "ffn")
DP_EXPERT_FFN = ("dp_0", "dp_1", "expert", "ffn")


def sent_together(arrays, axis, split_dim, concat_dim, along):
    widths = [a.shape[along] for a in arrays]
    both = jnp.concatenate(arrays, axis=along)
    whole = lax.all_to_all(both, axis, split_axis=split_dim, concat_axis=concat_dim, tiled=True)
    return tuple(jnp.split(whole, [sum(widths[:k]) for k in range(1, len(widths))], axis=along))


def side_by_side(arrays, axis, dim, along):
    both = jnp.concatenate(arrays, axis=along)
    whole, at, gathered = (lax.all_gather(both, axis, axis=dim, tiled=True), 0, [])
    for a in arrays:
        gathered.append(lax.slice_in_dim(whole, at, at + a.shape[along], axis=along))
        at += a.shape[along]
    return tuple(gathered)


def split_up(x, dim, devices):
    lengths = x.shape
    tiles = x.reshape(*lengths[:dim], devices, lengths[dim] // devices, *lengths[dim + 1 :])
    return jnp.moveaxis(tiles, dim, 0)


def sum_at_owner(x, axis, dim):
    devices = lax.axis_size(axis)
    tiles = lax.all_to_all(split_up(x, dim, devices), axis, 0, 0, tiled=True)
    return jnp.sum(tiles.astype(jnp.float32), axis=0)


def silu_parts(pre_act):
    sigmoid_value = jax.nn.sigmoid(pre_act)
    return (pre_act * sigmoid_value, sigmoid_value * (1.0 + pre_act * (1.0 - sigmoid_value)))


def against_rows(left_rows, right_rows):
    return lax.dot_general(
        left_rows, right_rows, (((0,), (0,)), ((), ())), preferred_element_type=jnp.float32
    )


def across_width(left_rows, weight):
    return lax.dot_general(
        left_rows, weight, (((1,), (1,)), ((), ())), preferred_element_type=jnp.float32
    )


def squares_of(matrix):
    return jnp.sum(matrix * matrix)


def on_device(tokens, expert_ids, route_weight, cotangent, w_gate, w_up, w_down):
    tok_rows, feature_width = tokens.shape
    experts = lax.axis_size("expert")
    groups = lax.axis_size(DP_FFN)
    capacity = tok_rows // 2
    slot_count = experts * capacity
    column_width = feature_width // groups
    chosen = expert_ids[:, :, None] == jnp.arange(experts, dtype=jnp.int32)[None, None, :]
    per_token = jnp.sum(chosen.astype(jnp.int32), axis=1)
    earlier = jnp.cumsum(per_token, axis=0) - per_token
    position = jnp.sum(jnp.where(chosen, earlier[:, None, :], 0), axis=2)
    slot_index = expert_ids * capacity + position
    slot_hot = slot_index[:, :, None] == jnp.arange(slot_count, dtype=jnp.int32)[None, None, :]
    hot_all = slot_hot.reshape(tok_rows * 2, slot_count).astype(jnp.bfloat16)
    scaled = (route_weight[:, :, None] * cotangent.astype(jnp.float32)[:, None, :]).astype(
        jnp.bfloat16
    )
    token_slots = against_rows(hot_all, jnp.repeat(tokens, 2, axis=0)).astype(jnp.bfloat16)
    grad_slots = against_rows(hot_all, scaled.reshape(tok_rows * 2, feature_width)).astype(
        jnp.bfloat16
    )
    token_cube = token_slots.reshape(experts, capacity, feature_width)
    grad_cube = grad_slots.reshape(experts, capacity, feature_width)
    column_start = lax.axis_index(DP_FFN) * column_width
    token_part = lax.dynamic_slice_in_dim(token_cube, column_start, column_width, 2)
    grad_part = lax.dynamic_slice_in_dim(grad_cube, column_start, column_width, 2)
    received = sent_together((token_part, grad_part), "expert", 0, 0, 1)
    slot_rows, slot_grads = side_by_side(
        (
            received[0].reshape(slot_count, column_width),
            received[1].reshape(slot_count, column_width),
        ),
        DP_FFN,
        1,
        0,
    )
    gate_weight = w_gate[0]
    up_weight = w_up[0]
    down_weight = w_down[0]
    pre_gate = across_width(slot_rows, gate_weight)
    pre_up = across_width(slot_rows, up_weight)
    activated, derivative = silu_parts(pre_gate)
    hidden = (activated * pre_up).astype(jnp.bfloat16)
    partial_value = jnp.dot(hidden, down_weight, preferred_element_type=jnp.float32)
    grad_down = against_rows(hidden, slot_grads)
    grad_hidden = across_width(slot_grads, down_weight)
    delta_gate = (grad_hidden * pre_up * derivative).astype(jnp.bfloat16)
    delta_up = (grad_hidden * activated).astype(jnp.bfloat16)
    grad_gate = against_rows(delta_gate, slot_rows)
    grad_up = against_rows(delta_up, slot_rows)
    sum_squares = lax.psum(
        squares_of(grad_gate) + squares_of(grad_up) + squares_of(grad_down), DP_EXPERT_FFN
    )
    summed = sum_at_owner(partial_value.astype(jnp.bfloat16), DP_FFN, 1).astype(jnp.bfloat16)
    summed = summed.reshape(experts, capacity, column_width)
    returned_rows = lax.all_to_all(
        summed, "expert", split_axis=0, concat_axis=0, tiled=True
    ).reshape(slot_count, column_width)
    picked = jnp.dot(hot_all, returned_rows, preferred_element_type=jnp.float32).reshape(
        tok_rows, 2, column_width
    )
    layer_out = jnp.sum(route_weight[:, :, None] * picked, axis=1).astype(jnp.bfloat16)
    inv_rms = lax.rsqrt(sum_squares / (3.0 * experts * FF * feature_width) + 1e-06)
    return (
        layer_out,
        (grad_gate * inv_rms).astype(jnp.bfloat16)[None],
        (grad_up * inv_rms).astype(jnp.bfloat16)[None],
        (grad_down * inv_rms).astype(jnp.bfloat16)[None],
    )


def solution(mesh):
    finer = Mesh(
        mesh.devices.reshape(4, 2, mesh.shape["expert"], mesh.shape["ffn"]),
        ("dp_0", "dp_1", "expert", "ffn"),
    )
    placed = (
        P("expert", None),
        P("expert", None),
        P("expert", None),
        P("expert", None),
        P("expert", DP_FFN, None),
        P("expert", DP_FFN, None),
        P("expert", DP_FFN, None),
    )
    return jax.shard_map(
        on_device,
        mesh=finer,
        in_specs=placed,
        out_specs=(
            P("expert", DP_FFN),
            P("expert", DP_FFN, None),
            P("expert", DP_FFN, None),
            P("expert", DP_FFN, None),
        ),
        check_vma=False,
    )
```

```python
import functools

import jax
import jax.numpy as jnp
from jax import lax
from jax.experimental import pallas as pl
from jax.experimental.pallas import tpu as pltpu
from jax.sharding import PartitionSpec as P

MESH = pl.DeviceIdType.MESH
BF = jnp.bfloat16
F32 = jnp.float32
LANES = 128
RING = 4
LEFT, RIGHT, FAR = 3, 1, 2
EVENTS = (
    ((0, 0),),
    ((LEFT, 0), (RIGHT, 0)),
    ((0, LEFT), (0, RIGHT)),
    ((FAR, 0),),
    ((LEFT, LEFT), (LEFT, RIGHT), (RIGHT, LEFT), (RIGHT, RIGHT)),
    ((0, FAR),),
    ((FAR, LEFT), (FAR, RIGHT)),
    ((LEFT, FAR), (RIGHT, FAR), (FAR, FAR)),
)


def dot(a, b, dims):
    return lax.dot_general(a, b, (dims, ((), ())), preferred_element_type=F32)


def body(
    ids, weight, tokens, cotangent, w_gate, w_up, w_down,
    gate_out, up_out, down_out, inv_out, layer_out,
    tok, cot, hot, hot_t, send, slots, w_gu, w_d, acc, hid_t, hid, delta, grads,
    psend, prem, part, relay, joined, half, last, final, back, sq_send, sq_recv,
    local, z_s, z_r, a_s, a_r, b_s, b_r, d_s, d_r, p_s, p_r, q_s, q_r, j_s, j_r,
    l_s, l_r, k_s, k_r, sq_s, sq_r,
    *, experts, total,
):
    dp, z, x = lax.axis_index("dp"), lax.axis_index("expert"), lax.axis_index("ffn")
    y, c = dp // 2, dp % 2
    cap = tok.shape[0] // 2
    count = experts * cap
    units = w_gate.shape[1]
    two, four = count // 2, count // 4

    def at(v, step):
        return (v + step) % RING

    def device(x_=x, y_=y, c_=c, z_=z):
        return {"dp": y_ * 2 + c_, "expert": z_, "ffn": x_}

    def slice_of(x_, y_, c_):
        return (2 * y_ + c_) * RING + x_

    started = []

    def put(src, dst, s_sem, r_sem, dev):
        copy = pltpu.make_async_remote_copy(
            src_ref=src, dst_ref=dst, send_sem=s_sem, recv_sem=r_sem, device_id=dev, device_id_type=MESH
        )
        copy.start()
        started.append(copy)

    def arrived(dst, s_sem, r_sem):
        pltpu.make_async_remote_copy(
            src_ref=dst, dst_ref=dst, send_sem=s_sem, recv_sem=r_sem,
            device_id=device(c_=1 - c), device_id_type=MESH,
        ).wait_recv()

    mine = slice_of(x, y, c)
    columns = pl.ds(pl.multiple_of(mine * LANES, LANES), LANES)
    loads = [
        pltpu.make_async_copy(tokens.at[:, columns], tok, local.at[0]),
        pltpu.make_async_copy(cotangent.at[:, columns], cot, local.at[1]),
        pltpu.make_async_copy(w_gate.at[0], w_gu.at[pl.ds(0, units)], local.at[2]),
        pltpu.make_async_copy(w_up.at[0], w_gu.at[pl.ds(units, units)], local.at[3]),
        pltpu.make_async_copy(w_down.at[0], w_d.at[pl.ds(0, units)], local.at[4]),
    ]
    for load in loads:
        load.start()

    peers = [device(c_=1 - c)]
    peers += [device(x_=at(x, s)) for s in (1, 2, 3)] + [device(y_=at(y, s)) for s in (1, 2, 3)]
    peers += [device(z_=(z + j) % experts) for j in range(1, experts)]
    barrier = pltpu.get_barrier_semaphore()
    for peer in peers:
        pl.semaphore_signal(barrier, inc=1, device_id=peer, device_id_type=MESH)

    rows = tok.shape[0]
    names = lax.broadcasted_iota(jnp.int32, (experts, rows), 0)
    chosen = [names == ids[k : k + 1, :] for k in (0, 1)]
    per_token = (chosen[0].astype(F32) + chosen[1].astype(F32)).astype(BF)
    before = (
        lax.broadcasted_iota(jnp.int32, (rows, rows), 0) < lax.broadcasted_iota(jnp.int32, (rows, rows), 1)
    ).astype(F32).astype(BF)
    earlier = dot(per_token, before, ((1,), (0,)))
    numbers = lax.broadcasted_iota(jnp.int32, (count, rows), 0).astype(F32)
    for k in (0, 1):
        position = jnp.sum(jnp.where(chosen[k], earlier, 0.0), axis=0, keepdims=True)
        slot = ids[k : k + 1, :].astype(F32) * float(cap) + position
        hot[k] = (numbers == slot).astype(F32).astype(BF)

    loads[0].wait()
    loads[1].wait()
    send[0] = dot(hot[0] + hot[1], tok[...], ((1,), (0,))).astype(BF)
    wide = cot[...].astype(F32)
    scaled = [(weight[:, k : k + 1] * wide).astype(BF) for k in (0, 1)]
    send[1] = (
        dot(hot[0], scaled[0], ((1,), (0,))) + dot(hot[1], scaled[1], ((1,), (0,)))
    ).astype(BF)
    own_rows = pl.ds(pl.multiple_of(z * cap, cap), cap)
    pl.semaphore_wait(barrier, len(peers))
    for j in range(1, experts):
        to = (z + j) % experts
        to_rows = pl.ds(pl.multiple_of(to * cap, cap), cap)
        for p in (0, 1):
            put(
                send.at[p, to_rows], slots.at[p, mine, own_rows],
                z_s.at[p, j - 1], z_r.at[p, j - 1], device(z_=to),
            )
    for p in (0, 1):
        slots[p, mine, own_rows, :] = send[p, own_rows, :]
    acc[...] = jnp.zeros_like(acc)
    pad = w_d.shape[0] - units
    if pad:
        w_d[pl.ds(units, pad), :] = jnp.zeros((pad, w_d.shape[1]), BF)
        hid_t[pl.ds(units, pad), :] = jnp.zeros((pad, count), BF)
    for k in (0, 1):
        hot_t[k] = hot[k].astype(F32).T.astype(BF)
    for load in loads[2:]:
        load.wait()
    for j in range(1, experts):
        source = (z + experts - j) % experts
        from_rows = pl.ds(pl.multiple_of(source * cap, cap), cap)
        for p in (0, 1):
            arrived(slots.at[p, mine, from_rows], z_s.at[p, j - 1], z_r.at[p, j - 1])

    def place(p, k, m):
        return (at(x, k), at(y, m)) if p == 0 else (at(x, m), at(y, k))

    def own_slice(p, k, m):
        return slice_of(*place(p, k, m), c)

    def along(p, stage, step):
        return device(x_=at(x, step)) if (p == 0) == (stage == 0) else device(y_=at(y, step))

    def whole(p, s):
        return slots.at[p, s]

    def part_of(p, s, h):
        return slots.at[p, s, pl.ds(h * two, two)]

    def both_ways(p, stage, s, s_sem, r_sem):
        for n, step in ((0, LEFT), (1, RIGHT)):
            put(whole(p, s), whole(p, s), s_sem(n), r_sem(n), along(p, stage, step))

    def onward(p, stage, s, step, s_sem, r_sem):
        n, h, to = (3, 0, RIGHT) if step == LEFT else (2, 1, LEFT)
        ref = part_of(p, s, h)
        put(ref, ref, s_sem(n), r_sem(n), along(p, stage, to))

    def sem_a(p):
        return (lambda n: a_s.at[p, n]), (lambda n: a_r.at[p, n])

    def sem_b(p, k):
        return (lambda n: b_s.at[p, k, n]), (lambda n: b_r.at[p, k, n])

    def await_slice(p, k, m):
        if (k, m) == (0, 0):
            return
        s = own_slice(p, k, m)
        step, (s_sem, r_sem) = (k, sem_a(p)) if m == 0 else (m, sem_b(p, k))
        if step == LEFT:
            arrived(whole(p, s), s_sem(1), r_sem(1))
        elif step == RIGHT:
            arrived(whole(p, s), s_sem(0), r_sem(0))
        else:
            arrived(part_of(p, s, 0), s_sem(3), r_sem(3))
            arrived(part_of(p, s, 1), s_sem(2), r_sem(2))

    def accumulate(p, k, m):
        x_, y_ = place(p, k, m)
        pair = [slice_of(x_, y_, e) for e in (0, 1)]
        cols = [pl.ds(pl.multiple_of(s * LANES, LANES), LANES) for s in pair]
        right = jnp.concatenate([slots[p, s] for s in pair], axis=1)
        if p == 0:
            left = jnp.concatenate([w_gu[:, d] for d in cols], axis=1)
            acc[pl.ds(0, 2 * units), :] += dot(left, right, ((1,), (1,)))
        else:
            left = jnp.concatenate([w_d[pl.ds(0, units), d] for d in cols], axis=1)
            acc[pl.ds(2 * units, units), :] += dot(left, right, ((1,), (1,)))

    def finish(event):
        for k, m in event:
            for p in (0, 1):
                x_, y_ = place(p, k, m)
                arrived(whole(p, slice_of(x_, y_, 1 - c)), d_s.at[p, k, m], d_r.at[p, k, m])
        for k, m in event:
            for p in (0, 1):
                accumulate(p, k, m)

    previous = None
    for event in EVENTS:
        for k, m in event:
            for p in (0, 1):
                await_slice(p, k, m)
                s = own_slice(p, k, m)
                if m == 0:
                    if k == 0:
                        both_ways(p, 0, s, *sem_a(p))
                    elif k != FAR:
                        onward(p, 0, s, k, *sem_a(p))
                elif m != FAR:
                    onward(p, 1, s, m, *sem_b(p, k))
        for k, m in event:
            for p in (0, 1):
                s = own_slice(p, k, m)
                if m == 0:
                    both_ways(p, 1, s, *sem_b(p, k))
                put(whole(p, s), whole(p, s), d_s.at[p, k, m], d_r.at[p, k, m], device(c_=1 - c))
        if previous is not None:
            finish(previous)
        previous = event
    finish(previous)

    block = 32

    def activate(i, carry):
        r = pl.multiple_of(i * block, block)
        gate = acc[pl.ds(r, block), :]
        up = acc[pl.ds(units + r, block), :]
        grad = acc[pl.ds(2 * units + r, block), :]
        s = jax.nn.sigmoid(gate)
        active = gate * s
        hid_t[pl.ds(r, block), :] = (active * up).astype(BF)
        delta[pl.ds(r, block), :] = (grad * up * (s * (1.0 + gate * (1.0 - s)))).astype(BF)
        delta[pl.ds(units + r, block), :] = (grad * active).astype(BF)
        return carry

    lax.fori_loop(0, units // block, activate, 0)
    for i in range(hid_t.shape[0] // LANES):
        r = pl.ds(i * LANES, LANES)
        hid[:, r] = hid_t[r, :].astype(F32).T.astype(BF)

    width = RING * LANES

    def terms(y_, c_):
        cols = pl.ds(pl.multiple_of((2 * y_ + c_) * width, width), width)
        return dot(hid[...], w_d[:, cols], ((1,), (0,)))

    def partner_terms(i, carry):
        t = terms(i, 1 - c)
        for n in range(RING):
            psend[i, n] = t[:, n * LANES : (n + 1) * LANES].astype(BF)
        return carry

    lax.fori_loop(0, RING, partner_terms, 0)
    for i in range(RING):
        put(psend.at[i], prem.at[i], p_s.at[i], p_r.at[i], device(c_=1 - c))
    for i in range(RING):
        arrived(prem.at[i], p_s.at[i], p_r.at[i])

    def own_terms(i, carry):
        t = terms(i, c)
        for n in range(RING):
            part[i, n] = (t[:, n * LANES : (n + 1) * LANES] + prem[i, n].astype(F32)).astype(BF)
        return carry

    lax.fori_loop(0, RING, own_terms, 0)

    def view(h, t, start, size):
        r = pl.ds(h * two + start, size)
        return (slice(None), t, r, slice(None)) if h == 0 else (t, slice(None), r, slice(None))

    first = [x, y]
    second = [y, x]

    def hop(h, stage, step):
        return device(x_=at(x, step)) if (h == 0) == (stage == 0) else device(y_=at(y, step))

    for h in (0, 1):
        far = at(first[h], FAR)
        put(part.at[view(h, far, 0, four)], relay.at[h, 0], q_s.at[h, 0], q_r.at[h, 0], hop(h, 0, RIGHT))
        put(part.at[view(h, far, four, four)], relay.at[h, 1], q_s.at[h, 1], q_r.at[h, 1], hop(h, 0, LEFT))
    for h in (0, 1):
        put(
            part.at[view(h, at(first[h], RIGHT), four, four)], joined.at[h, 0, :, pl.ds(four, four)],
            j_s.at[h, 0, 0], j_r.at[h, 0, 0], hop(h, 0, RIGHT),
        )
        put(
            part.at[view(h, at(first[h], LEFT), 0, four)], joined.at[h, 1, :, pl.ds(0, four)],
            j_s.at[h, 1, 0], j_r.at[h, 1, 0], hop(h, 0, LEFT),
        )

    def gradients(i, squares):
        pair = [2 * i, 2 * i + 1]
        cols = pl.ds(pl.multiple_of(i * 2 * LANES, 2 * LANES), 2 * LANES)
        xs = jnp.concatenate([slots[0, s] for s in pair], axis=1)
        gs = jnp.concatenate([slots[1, s] for s in pair], axis=1)
        g = dot(delta[...], xs, ((1,), (0,)))
        grads[pl.ds(0, 2 * units), cols] = g.astype(BF)
        squares += jnp.sum((g * g).reshape(2 * units // 8, 8, 2 * LANES), axis=0)
        g = dot(hid_t[pl.ds(0, units), :], gs, ((1,), (0,)))
        grads[pl.ds(2 * units, units), cols] = g.astype(BF)
        return squares + jnp.sum((g * g).reshape(units // 8, 8, 2 * LANES), axis=0)

    pairs = slots.shape[1] // 2
    squares = lax.fori_loop(0, pairs // 2, gradients, jnp.zeros((8, 2 * LANES), F32))

    for h in (0, 1):
        arrived(relay.at[h, 0], q_s.at[h, 0], q_r.at[h, 0])
        v = view(h, at(first[h], RIGHT), 0, four)
        part[v] = (part[v].astype(F32) + relay[h, 0].astype(F32)).astype(BF)
        arrived(relay.at[h, 1], q_s.at[h, 1], q_r.at[h, 1])
        u = view(h, at(first[h], LEFT), four, four)
        part[u] = (part[u].astype(F32) + relay[h, 1].astype(F32)).astype(BF)
        put(part.at[v], joined.at[h, 0, :, pl.ds(0, four)], j_s.at[h, 0, 1], j_r.at[h, 0, 1], hop(h, 0, RIGHT))
        put(part.at[u], joined.at[h, 1, :, pl.ds(four, four)], j_s.at[h, 1, 1], j_r.at[h, 1, 1], hop(h, 0, LEFT))

    squares = lax.fori_loop(pairs // 2, pairs, gradients, squares)
    stores = [
        pltpu.make_async_copy(grads.at[pl.ds(n * units, units)], out, local.at[5 + n])
        for n, out in enumerate((gate_out, up_out, down_out))
    ]
    for store in stores:
        store.start()

    def share(stage, value, devices, base):
        sq_send[stage] = value
        for n, dev in enumerate(devices):
            put(sq_send.at[stage], sq_recv.at[base + n], sq_s.at[base + n], sq_r.at[base + n], dev)

    def gathered(value, base, n):
        for i in range(base, base + n):
            arrived(sq_recv.at[i], sq_s.at[i], sq_r.at[i])
            value = value + sq_recv[i]
        return value

    value = squares[:, :LANES] + squares[:, LANES:]
    share(0, value, [device(c_=1 - c)], 0)

    for h in (0, 1):
        for n, starts in enumerate(((four, 0), (0, four))):
            for piece, start in enumerate(starts):
                arrived(joined.at[h, n, :, pl.ds(start, four)], j_s.at[h, n, piece], j_r.at[h, n, piece])
        v = view(h, first[h], 0, two)
        half[h] = (part[v].astype(F32) + joined[h, 0].astype(F32) + joined[h, 1].astype(F32)).astype(BF)
        for j in (1, 2, 3):
            put(half.at[h, at(second[h], j)], last.at[h, j - 1], l_s.at[h, j - 1], l_r.at[h, j - 1], hop(h, 1, j))
    value = gathered(value, 0, 1)
    share(1, value, [device(x_=at(x, s)) for s in (1, 2, 3)], 1)

    for h in (0, 1):
        summed = half[h, second[h]].astype(F32)
        for j in (1, 2, 3):
            arrived(last.at[h, j - 1], l_s.at[h, j - 1], l_r.at[h, j - 1])
            summed = summed + last[h, j - 1].astype(F32)
        final[pl.ds(h * two, two), :] = summed.astype(BF)
    for j in range(1, experts):
        to = (z + j) % experts
        to_rows = pl.ds(pl.multiple_of(to * cap, cap), cap)
        put(final.at[to_rows], back.at[own_rows], k_s.at[j - 1], k_r.at[j - 1], device(z_=to))
    value = gathered(value, 1, 3)
    share(2, value, [device(y_=at(y, s)) for s in (1, 2, 3)], 4)
    back[own_rows, :] = final[own_rows, :]
    value = gathered(value, 4, 3)
    share(3, value, [device(z_=(z + j) % experts) for j in range(1, experts)], 7)
    for j in range(1, experts):
        source = (z + experts - j) % experts
        from_rows = pl.ds(pl.multiple_of(source * cap, cap), cap)
        arrived(back.at[from_rows], k_s.at[j - 1], k_r.at[j - 1])
    picked = [dot(hot_t[k], back[...], ((1,), (0,))) for k in (0, 1)]
    layer_out[...] = (weight[:, 0:1] * picked[0] + weight[:, 1:2] * picked[1]).astype(BF)
    value = gathered(value, 7, experts - 1)
    inv_out[...] = jnp.broadcast_to(
        lax.rsqrt(jnp.sum(value, keepdims=True) / total + 1e-06), inv_out.shape
    )
    for store in stores:
        store.wait()
    for copy in started:
        copy.wait_send()


def solution(mesh):
    experts = mesh.shape["expert"]
    groups = mesh.shape["dp"] * mesh.shape["ffn"]

    def on_device(tokens, expert_ids, route_weight, cotangent, w_gate, w_up, w_down):
        rows, features = tokens.shape
        units = w_gate.shape[1]
        padded = -(-units // LANES) * LANES
        count = experts * rows // 2
        two, four = count // 2, count // 4
        total = 3.0 * experts * units * groups * features
        vmem, anywhere = pl.BlockSpec(memory_space=pltpu.VMEM), pl.BlockSpec(memory_space=pl.ANY)
        dma = pltpu.SemaphoreType.DMA
        gate, up, down, inv, layer = pl.pallas_call(
            functools.partial(body, experts=experts, total=total),
            out_shape=[jax.ShapeDtypeStruct((units, features), BF)] * 3
            + [jax.ShapeDtypeStruct((8, LANES), F32), jax.ShapeDtypeStruct((rows, LANES), BF)],
            in_specs=[vmem, vmem] + [anywhere] * 5,
            out_specs=[anywhere] * 3 + [vmem, vmem],
            scratch_shapes=[
                pltpu.VMEM((rows, LANES), BF),
                pltpu.VMEM((rows, LANES), BF),
                pltpu.VMEM((2, count, rows), BF),
                pltpu.VMEM((2, rows, count), BF),
                pltpu.VMEM((2, count, LANES), BF),
                pltpu.VMEM((2, groups, count, LANES), BF),
                pltpu.VMEM((2 * units, features), BF),
                pltpu.VMEM((padded, features), BF),
                pltpu.VMEM((3 * units, count), F32),
                pltpu.VMEM((padded, count), BF),
                pltpu.VMEM((count, padded), BF),
                pltpu.VMEM((2 * units, count), BF),
                pltpu.VMEM((3 * units, features), BF),
                pltpu.VMEM((RING, RING, count, LANES), BF),
                pltpu.VMEM((RING, RING, count, LANES), BF),
                pltpu.VMEM((RING, RING, count, LANES), BF),
                pltpu.VMEM((2, 2, RING, four, LANES), BF),
                pltpu.VMEM((2, 2, RING, two, LANES), BF),
                pltpu.VMEM((2, RING, two, LANES), BF),
                pltpu.VMEM((2, 3, two, LANES), BF),
                pltpu.VMEM((count, LANES), BF),
                pltpu.VMEM((count, LANES), BF),
                pltpu.VMEM((4, 8, LANES), F32),
                pltpu.VMEM((6 + experts, 8, LANES), F32),
                dma((8,)),
                dma((2, experts - 1)), dma((2, experts - 1)),
                dma((2, 4)), dma((2, 4)),
                dma((2, RING, 4)), dma((2, RING, 4)),
                dma((2, RING, RING)), dma((2, RING, RING)),
                dma((RING,)), dma((RING,)),
                dma((2, 2)), dma((2, 2)),
                dma((2, 2, 2)), dma((2, 2, 2)),
                dma((2, 3)), dma((2, 3)),
                dma((experts - 1,)), dma((experts - 1,)),
                dma((6 + experts,)), dma((6 + experts,)),
            ],
            compiler_params=pltpu.CompilerParams(
                collective_id=0, has_side_effects=True, vmem_limit_bytes=60 * 1024 * 1024
            ),
            name="layer",
        )(expert_ids.T, route_weight, tokens, cotangent, w_gate, w_up, w_down)
        scale = inv[0, 0]
        return (
            layer,
            (gate.astype(F32) * scale).astype(BF)[None],
            (up.astype(F32) * scale).astype(BF)[None],
            (down.astype(F32) * scale).astype(BF)[None],
        )

    token, hidden = P("expert", None), P("expert", ("dp", "ffn"), None)
    return jax.shard_map(
        on_device,
        mesh=mesh,
        in_specs=(token, token, token, token, hidden, hidden, hidden),
        out_specs=(P("expert", ("dp", "ffn")), hidden, hidden, hidden),
        check_vma=False,
    )
```

```python
import functools

import jax
import jax.numpy as jnp
from jax import lax
from jax.experimental import pallas as pl
from jax.experimental.pallas import tpu as pltpu
from jax.sharding import PartitionSpec as P

MESH = pl.DeviceIdType.MESH
BF = jnp.bfloat16
F32 = jnp.float32
LANES = 128
BLOCK = 32
VMEM = 36 * 1024 * 1024
SCALE_VMEM = 20 * 1024 * 1024
RING = 4
LEFT, RIGHT, FAR = 3, 1, 2
EVENTS = (
    ((0, 0),),
    ((LEFT, 0), (RIGHT, 0)),
    ((0, LEFT), (0, RIGHT)),
    ((FAR, 0),),
    ((LEFT, LEFT), (LEFT, RIGHT), (RIGHT, LEFT), (RIGHT, RIGHT)),
    ((0, FAR),),
    ((FAR, LEFT), (FAR, RIGHT)),
    ((LEFT, FAR), (RIGHT, FAR), (FAR, FAR)),
)


def dot(a, b, dims):
    return lax.dot_general(a, b, (dims, ((), ())), preferred_element_type=F32)


def body(
    ids, weight, tokens, cotangent, w_gate, w_up, w_down,
    grads, inv_out, layer_out,
    tok, cot, hot, hot_t, send, slots, w_gu, w_d, acc, hid_t, hid, delta, weights,
    psend, prem, part, relay, joined, half, last, final, back, sq_send, sq_recv,
    local, z_s, z_r, a_s, a_r, b_s, b_r, d_s, d_r, p_s, p_r, q_s, q_r, j_s, j_r,
    l_s, l_r, k_s, k_r, sq_s, sq_r,
    *, experts, total,
):
    dp, z, x = lax.axis_index("dp"), lax.axis_index("expert"), lax.axis_index("ffn")
    y, c = dp // 2, dp % 2
    cap = tok.shape[0] // 2
    count = experts * cap
    units = w_gate.shape[1]
    two, four = count // 2, count // 4

    def at(v, step):
        return (v + step) % RING

    def device(x_=x, y_=y, c_=c, z_=z):
        return {"dp": y_ * 2 + c_, "expert": z_, "ffn": x_}

    def slice_of(x_, y_, c_):
        return (2 * y_ + c_) * RING + x_

    started = []

    def put(src, dst, s_sem, r_sem, dev):
        copy = pltpu.make_async_remote_copy(
            src_ref=src, dst_ref=dst, send_sem=s_sem, recv_sem=r_sem, device_id=dev, device_id_type=MESH
        )
        copy.start()
        started.append(copy)

    def arrived(dst, s_sem, r_sem):
        pltpu.make_async_remote_copy(
            src_ref=dst, dst_ref=dst, send_sem=s_sem, recv_sem=r_sem,
            device_id=device(c_=1 - c), device_id_type=MESH,
        ).wait_recv()

    mine = slice_of(x, y, c)
    columns = pl.ds(pl.multiple_of(mine * LANES, LANES), LANES)
    loads = [
        pltpu.make_async_copy(tokens.at[:, columns], tok, local.at[0]),
        pltpu.make_async_copy(cotangent.at[:, columns], cot, local.at[1]),
        pltpu.make_async_copy(w_gate.at[0], w_gu.at[pl.ds(0, units)], local.at[2]),
        pltpu.make_async_copy(w_up.at[0], w_gu.at[pl.ds(units, units)], local.at[3]),
        pltpu.make_async_copy(w_down.at[0], w_d.at[pl.ds(0, units)], local.at[4]),
    ]
    for load in loads:
        load.start()

    peers = [device(c_=1 - c)]
    peers += [device(x_=at(x, s)) for s in (1, 2, 3)] + [device(y_=at(y, s)) for s in (1, 2, 3)]
    peers += [device(z_=(z + j) % experts) for j in range(1, experts)]
    barrier = pltpu.get_barrier_semaphore()
    for peer in peers:
        pl.semaphore_signal(barrier, inc=1, device_id=peer, device_id_type=MESH)

    rows = tok.shape[0]
    names = lax.broadcasted_iota(jnp.int32, (experts, rows), 0)
    chosen = [names == ids[k : k + 1, :] for k in (0, 1)]
    per_token = (chosen[0].astype(F32) + chosen[1].astype(F32)).astype(BF)
    before = (
        lax.broadcasted_iota(jnp.int32, (rows, rows), 0) < lax.broadcasted_iota(jnp.int32, (rows, rows), 1)
    ).astype(F32).astype(BF)
    earlier = dot(per_token, before, ((1,), (0,)))
    numbers = lax.broadcasted_iota(jnp.int32, (count, rows), 0).astype(F32)
    for k in (0, 1):
        position = jnp.sum(jnp.where(chosen[k], earlier, 0.0), axis=0, keepdims=True)
        slot = ids[k : k + 1, :].astype(F32) * float(cap) + position
        hot[k] = (numbers == slot).astype(F32).astype(BF)

    loads[0].wait()
    loads[1].wait()
    send[0] = dot(hot[0] + hot[1], tok[...], ((1,), (0,))).astype(BF)
    wide = cot[...].astype(F32)
    for k in (0, 1):
        weights[k] = jnp.broadcast_to(weight[k : k + 1, :], (LANES, rows)).T
    scaled = [(weights[k] * wide).astype(BF) for k in (0, 1)]
    send[1] = (
        dot(hot[0], scaled[0], ((1,), (0,))) + dot(hot[1], scaled[1], ((1,), (0,)))
    ).astype(BF)
    own_rows = pl.ds(pl.multiple_of(z * cap, cap), cap)
    pl.semaphore_wait(barrier, len(peers))
    for p in (0, 1):
        for j in sorted(range(1, experts), key=lambda j: -min(j, experts - j)):
            to = (z + j) % experts
            to_rows = pl.ds(pl.multiple_of(to * cap, cap), cap)
            put(
                send.at[p, to_rows], slots.at[p, mine, own_rows],
                z_s.at[p, j - 1], z_r.at[p, j - 1], device(z_=to),
            )
    for p in (0, 1):
        slots[p, mine, own_rows, :] = send[p, own_rows, :]
    acc[...] = jnp.zeros_like(acc)
    pad = w_d.shape[0] - units
    if pad:
        w_d[pl.ds(units, pad), :] = jnp.zeros((pad, w_d.shape[1]), BF)
        hid_t[pl.ds(units, pad), :] = jnp.zeros((pad, count), BF)
    for k in (0, 1):
        hot_t[k] = hot[k].astype(F32).T.astype(BF)
    for load in loads[2:]:
        load.wait()

    def await_tokens(p):
        for j in range(1, experts):
            source = (z + experts - j) % experts
            from_rows = pl.ds(pl.multiple_of(source * cap, cap), cap)
            arrived(slots.at[p, mine, from_rows], z_s.at[p, j - 1], z_r.at[p, j - 1])

    def place(p, k, m):
        return (at(x, k), at(y, m)) if p == 0 else (at(x, m), at(y, k))

    def own_slice(p, k, m):
        return slice_of(*place(p, k, m), c)

    def along(p, stage, step):
        return device(x_=at(x, step)) if (p == 0) == (stage == 0) else device(y_=at(y, step))

    def whole(p, s):
        return slots.at[p, s]

    def part_of(p, s, h):
        return slots.at[p, s, pl.ds(h * two, two)]

    def both_ways(p, stage, s, s_sem, r_sem):
        for n, step in ((0, LEFT), (1, RIGHT)):
            put(whole(p, s), whole(p, s), s_sem(n), r_sem(n), along(p, stage, step))

    def onward(p, stage, s, step, s_sem, r_sem):
        n, h, to = (3, 0, RIGHT) if step == LEFT else (2, 1, LEFT)
        ref = part_of(p, s, h)
        put(ref, ref, s_sem(n), r_sem(n), along(p, stage, to))

    def sem_a(p):
        return (lambda n: a_s.at[p, n]), (lambda n: a_r.at[p, n])

    def sem_b(p, k):
        return (lambda n: b_s.at[p, k, n]), (lambda n: b_r.at[p, k, n])

    def await_slice(p, k, m):
        if (k, m) == (0, 0):
            return
        s = own_slice(p, k, m)
        step, (s_sem, r_sem) = (k, sem_a(p)) if m == 0 else (m, sem_b(p, k))
        if step == LEFT:
            arrived(whole(p, s), s_sem(1), r_sem(1))
        elif step == RIGHT:
            arrived(whole(p, s), s_sem(0), r_sem(0))
        else:
            arrived(part_of(p, s, 0), s_sem(3), r_sem(3))
            arrived(part_of(p, s, 1), s_sem(2), r_sem(2))

    def accumulate(p, k, m):
        x_, y_ = place(p, k, m)
        pair = [slice_of(x_, y_, e) for e in (0, 1)]
        cols = [pl.ds(pl.multiple_of(s * LANES, LANES), LANES) for s in pair]
        right = jnp.concatenate([slots[p, s] for s in pair], axis=1)
        if p == 0:
            left = jnp.concatenate([w_gu[:, d] for d in cols], axis=1)
            acc[pl.ds(0, 2 * units), :] += dot(left, right, ((1,), (1,)))
        else:
            left = jnp.concatenate([w_d[pl.ds(0, units), d] for d in cols], axis=1)
            acc[pl.ds(2 * units, units), :] += dot(left, right, ((1,), (1,)))

    def finish(event):
        for k, m in event:
            for p in (0, 1):
                x_, y_ = place(p, k, m)
                arrived(whole(p, slice_of(x_, y_, 1 - c)), d_s.at[p, k, m], d_r.at[p, k, m])
        for k, m in event:
            for p in (0, 1):
                accumulate(p, k, m)

    def take(p, k, m):
        await_slice(p, k, m)
        s = own_slice(p, k, m)
        if m == 0:
            if k == 0:
                both_ways(p, 0, s, *sem_a(p))
            elif k != FAR:
                onward(p, 0, s, k, *sem_a(p))
        elif m != FAR:
            onward(p, 1, s, m, *sem_b(p, k))

    def pass_on(p, k, m):
        s = own_slice(p, k, m)
        if m == 0:
            both_ways(p, 1, s, *sem_b(p, k))
        put(whole(p, s), whole(p, s), d_s.at[p, k, m], d_r.at[p, k, m], device(c_=1 - c))

    for p in (0, 1):
        await_tokens(p)
        take(p, 0, 0)
        pass_on(p, 0, 0)
    previous = EVENTS[0]
    for event in EVENTS[1:]:
        for k, m in event:
            for p in (0, 1):
                take(p, k, m)
        for k, m in event:
            for p in (0, 1):
                pass_on(p, k, m)
        finish(previous)
        previous = event
    finish(previous)

    block = BLOCK

    def activate(i, carry):
        r = pl.multiple_of(i * block, block)
        gate = acc[pl.ds(r, block), :]
        up = acc[pl.ds(units + r, block), :]
        grad = acc[pl.ds(2 * units + r, block), :]
        s = jax.nn.sigmoid(gate)
        active = gate * s
        hid_t[pl.ds(r, block), :] = (active * up).astype(BF)
        delta[pl.ds(r, block), :] = (grad * up * (s * (1.0 + gate * (1.0 - s)))).astype(BF)
        delta[pl.ds(units + r, block), :] = (grad * active).astype(BF)
        return carry

    lax.fori_loop(0, units // block, activate, 0)
    for i in range(hid_t.shape[0] // LANES):
        r = pl.ds(i * LANES, LANES)
        hid[:, r] = hid_t[r, :].astype(F32).T.astype(BF)

    width = RING * LANES

    def terms(y_, c_):
        cols = pl.ds(pl.multiple_of((2 * y_ + c_) * width, width), width)
        return dot(hid[...], w_d[:, cols], ((1,), (0,)))

    for i in range(RING):
        t = terms(i, 1 - c)
        for n in range(RING):
            psend[i, n] = t[:, n * LANES : (n + 1) * LANES].astype(BF)
        put(psend.at[i], prem.at[i], p_s.at[i], p_r.at[i], device(c_=1 - c))
    for i in range(RING):
        t = terms(i, c)
        arrived(prem.at[i], p_s.at[i], p_r.at[i])
        for n in range(RING):
            part[i, n] = (t[:, n * LANES : (n + 1) * LANES] + prem[i, n].astype(F32)).astype(BF)

    def view(h, t, start, size):
        r = pl.ds(h * two + start, size)
        return (slice(None), t, r, slice(None)) if h == 0 else (t, slice(None), r, slice(None))

    first = [x, y]
    second = [y, x]

    def hop(h, stage, step):
        return device(x_=at(x, step)) if (h == 0) == (stage == 0) else device(y_=at(y, step))

    for h in (0, 1):
        far = at(first[h], FAR)
        put(part.at[view(h, far, 0, four)], relay.at[h, 0], q_s.at[h, 0], q_r.at[h, 0], hop(h, 0, RIGHT))
        put(part.at[view(h, far, four, four)], relay.at[h, 1], q_s.at[h, 1], q_r.at[h, 1], hop(h, 0, LEFT))
    for h in (0, 1):
        put(
            part.at[view(h, at(first[h], RIGHT), four, four)], joined.at[h, 0, :, pl.ds(four, four)],
            j_s.at[h, 0, 0], j_r.at[h, 0, 0], hop(h, 0, RIGHT),
        )
        put(
            part.at[view(h, at(first[h], LEFT), 0, four)], joined.at[h, 1, :, pl.ds(0, four)],
            j_s.at[h, 1, 0], j_r.at[h, 1, 0], hop(h, 0, LEFT),
        )

    def gradients(i, squares):
        pair = [2 * i, 2 * i + 1]
        cols = pl.ds(pl.multiple_of(i * 2 * LANES, 2 * LANES), 2 * LANES)
        xs = jnp.concatenate([slots[0, s] for s in pair], axis=1)
        gs = jnp.concatenate([slots[1, s] for s in pair], axis=1)
        g = dot(delta[...], xs, ((1,), (0,)))
        grads[pl.ds(0, 2 * units), cols] = g
        squares += jnp.sum((g * g).reshape(2 * units // 8, 8, 2 * LANES), axis=0)
        g = dot(hid_t[pl.ds(0, units), :], gs, ((1,), (0,)))
        grads[pl.ds(2 * units, units), cols] = g
        return squares + jnp.sum((g * g).reshape(units // 8, 8, 2 * LANES), axis=0)

    pairs = slots.shape[1] // 2
    squares = lax.fori_loop(0, pairs // 2, gradients, jnp.zeros((8, 2 * LANES), F32))

    for h in (0, 1):
        arrived(relay.at[h, 0], q_s.at[h, 0], q_r.at[h, 0])
        v = view(h, at(first[h], RIGHT), 0, four)
        part[v] = (part[v].astype(F32) + relay[h, 0].astype(F32)).astype(BF)
        arrived(relay.at[h, 1], q_s.at[h, 1], q_r.at[h, 1])
        u = view(h, at(first[h], LEFT), four, four)
        part[u] = (part[u].astype(F32) + relay[h, 1].astype(F32)).astype(BF)
        put(part.at[v], joined.at[h, 0, :, pl.ds(0, four)], j_s.at[h, 0, 1], j_r.at[h, 0, 1], hop(h, 0, RIGHT))
        put(part.at[u], joined.at[h, 1, :, pl.ds(four, four)], j_s.at[h, 1, 1], j_r.at[h, 1, 1], hop(h, 0, LEFT))

    squares = lax.fori_loop(pairs // 2, pairs, gradients, squares)

    def share(stage, value, devices, base):
        sq_send[stage] = value
        for n, dev in enumerate(devices):
            put(sq_send.at[stage], sq_recv.at[base + n], sq_s.at[base + n], sq_r.at[base + n], dev)

    def gathered(value, base, n):
        for i in range(base, base + n):
            arrived(sq_recv.at[i], sq_s.at[i], sq_r.at[i])
            value = value + sq_recv[i]
        return value

    value = squares[:, :LANES] + squares[:, LANES:]
    share(0, value, [device(c_=1 - c)], 0)

    for h in (0, 1):
        for n, starts in enumerate(((four, 0), (0, four))):
            for piece, start in enumerate(starts):
                arrived(joined.at[h, n, :, pl.ds(start, four)], j_s.at[h, n, piece], j_r.at[h, n, piece])
        v = view(h, first[h], 0, two)
        half[h] = (part[v].astype(F32) + joined[h, 0].astype(F32) + joined[h, 1].astype(F32)).astype(BF)
        for j in (1, 2, 3):
            put(half.at[h, at(second[h], j)], last.at[h, j - 1], l_s.at[h, j - 1], l_r.at[h, j - 1], hop(h, 1, j))
    value = gathered(value, 0, 1)
    share(1, value, [device(x_=at(x, s)) for s in (1, 2, 3)], 1)

    for h in (0, 1):
        summed = half[h, second[h]].astype(F32)
        for j in (1, 2, 3):
            arrived(last.at[h, j - 1], l_s.at[h, j - 1], l_r.at[h, j - 1])
            summed = summed + last[h, j - 1].astype(F32)
        final[pl.ds(h * two, two), :] = summed.astype(BF)
    for j in range(1, experts):
        to = (z + j) % experts
        to_rows = pl.ds(pl.multiple_of(to * cap, cap), cap)
        put(final.at[to_rows], back.at[own_rows], k_s.at[j - 1], k_r.at[j - 1], device(z_=to))
    value = gathered(value, 1, 3)
    share(2, value, [device(y_=at(y, s)) for s in (1, 2, 3)], 4)
    back[own_rows, :] = final[own_rows, :]
    value = gathered(value, 4, 3)
    share(3, value, [device(z_=(z + j) % experts) for j in range(1, experts)], 7)
    for j in range(1, experts):
        source = (z + experts - j) % experts
        from_rows = pl.ds(pl.multiple_of(source * cap, cap), cap)
        arrived(back.at[from_rows], k_s.at[j - 1], k_r.at[j - 1])
    picked = [dot(hot_t[k], back[...], ((1,), (0,))) for k in (0, 1)]
    layer_out[...] = (weights[0] * picked[0] + weights[1] * picked[1]).astype(BF)
    value = gathered(value, 7, experts - 1)
    inv_out[...] = jnp.broadcast_to(
        lax.rsqrt(jnp.sum(value, keepdims=True) / total + 1e-06), inv_out.shape
    )
    for copy in started:
        copy.wait_send()


def scale_body(grads, inv, layer, gate_out, up_out, down_out, layer_out, scaled, sems):
    units = gate_out.shape[0]
    blocks = units // BLOCK
    scale = inv[0:1, 0:1]
    for n, out in enumerate((gate_out, up_out, down_out)):

        def step(i, carry):
            r = pl.multiple_of(i * BLOCK, BLOCK)
            rows = pl.ds(n * units + r, BLOCK)
            scaled[rows, :] = (grads[rows, :] * scale).astype(BF)
            pltpu.make_async_copy(scaled.at[rows], out.at[pl.ds(r, BLOCK)], sems.at[n * blocks + i]).start()
            return carry

        lax.fori_loop(0, blocks, step, 0)
    layer_out[...] = layer[...]
    for n, out in enumerate((gate_out, up_out, down_out)):
        for i in range(blocks):
            rows = pl.ds(n * units + i * BLOCK, BLOCK)
            pltpu.make_async_copy(scaled.at[rows], out.at[pl.ds(i * BLOCK, BLOCK)], sems.at[n * blocks + i]).wait()


def solution(mesh):
    experts = mesh.shape["expert"]
    groups = mesh.shape["dp"] * mesh.shape["ffn"]

    def on_device(tokens, expert_ids, route_weight, cotangent, w_gate, w_up, w_down):
        rows, features = tokens.shape
        units = w_gate.shape[1]
        padded = -(-units // LANES) * LANES
        count = experts * rows // 2
        two, four = count // 2, count // 4
        total = 3.0 * experts * units * groups * features
        vmem, anywhere = pl.BlockSpec(memory_space=pltpu.VMEM), pl.BlockSpec(memory_space=pltpu.HBM)
        dma = pltpu.SemaphoreType.DMA
        grads, inv, layer = pl.pallas_call(
            functools.partial(body, experts=experts, total=total),
            out_shape=[
                jax.ShapeDtypeStruct((3 * units, features), F32),
                jax.ShapeDtypeStruct((8, LANES), F32),
                jax.ShapeDtypeStruct((rows, LANES), BF),
            ],
            in_specs=[vmem, vmem] + [anywhere] * 5,
            out_specs=[vmem] * 3,
            scratch_shapes=[
                pltpu.VMEM((rows, LANES), BF),
                pltpu.VMEM((rows, LANES), BF),
                pltpu.VMEM((2, count, rows), BF),
                pltpu.VMEM((2, rows, count), BF),
                pltpu.VMEM((2, count, LANES), BF),
                pltpu.VMEM((2, groups, count, LANES), BF),
                pltpu.VMEM((2 * units, features), BF),
                pltpu.VMEM((padded, features), BF),
                pltpu.VMEM((3 * units, count), F32),
                pltpu.VMEM((padded, count), BF),
                pltpu.VMEM((count, padded), BF),
                pltpu.VMEM((2 * units, count), BF),
                pltpu.VMEM((2, rows, LANES), F32),
                pltpu.VMEM((RING, RING, count, LANES), BF),
                pltpu.VMEM((RING, RING, count, LANES), BF),
                pltpu.VMEM((RING, RING, count, LANES), BF),
                pltpu.VMEM((2, 2, RING, four, LANES), BF),
                pltpu.VMEM((2, 2, RING, two, LANES), BF),
                pltpu.VMEM((2, RING, two, LANES), BF),
                pltpu.VMEM((2, 3, two, LANES), BF),
                pltpu.VMEM((count, LANES), BF),
                pltpu.VMEM((count, LANES), BF),
                pltpu.VMEM((4, 8, LANES), F32),
                pltpu.VMEM((6 + experts, 8, LANES), F32),
                dma((5,)),
                dma((2, experts - 1)), dma((2, experts - 1)),
                dma((2, 4)), dma((2, 4)),
                dma((2, RING, 4)), dma((2, RING, 4)),
                dma((2, RING, RING)), dma((2, RING, RING)),
                dma((RING,)), dma((RING,)),
                dma((2, 2)), dma((2, 2)),
                dma((2, 2, 2)), dma((2, 2, 2)),
                dma((2, 3)), dma((2, 3)),
                dma((experts - 1,)), dma((experts - 1,)),
                dma((6 + experts,)), dma((6 + experts,)),
            ],
            compiler_params=pltpu.CompilerParams(
                collective_id=0, has_side_effects=True, vmem_limit_bytes=VMEM
            ),
            name="layer",
        )(expert_ids.T, route_weight.T, *[pltpu.with_memory_space_constraint(a, pltpu.HBM) for a in (tokens, cotangent, w_gate, w_up, w_down)])
        gate, up, down, layer = pl.pallas_call(
            scale_body,
            out_shape=[jax.ShapeDtypeStruct((units, features), BF)] * 3
            + [jax.ShapeDtypeStruct((rows, LANES), BF)],
            in_specs=[vmem] * 3,
            out_specs=[anywhere] * 3 + [vmem],
            scratch_shapes=[pltpu.VMEM((3 * units, features), BF), dma((3 * (units // BLOCK),))],
            compiler_params=pltpu.CompilerParams(vmem_limit_bytes=SCALE_VMEM),
            name="scale",
        )(grads, inv, layer)
        return layer, gate[None], up[None], down[None]

    token, hidden = P("expert", None), P("expert", ("dp", "ffn"), None)
    return jax.shard_map(
        on_device,
        mesh=mesh,
        in_specs=(token, token, token, token, hidden, hidden, hidden),
        out_specs=(P("expert", ("dp", "ffn")), hidden, hidden, hidden),
        check_vma=False,
    )
```

```python
import functools

import jax
import jax.numpy as jnp
from jax import lax
from jax.experimental import pallas as pl
from jax.experimental.pallas import tpu as pltpu
from jax.sharding import PartitionSpec as P

MESH = pl.DeviceIdType.MESH
BF = jnp.bfloat16
F32 = jnp.float32
LANES = 128
BLOCK = 32
VMEM = 46 * 1024 * 1024
COPY_VMEM = 4 * 1024 * 1024
RING = 4
LEFT, RIGHT, FAR = 3, 1, 2
EVENTS = (
    ((0, 0),),
    ((LEFT, 0), (RIGHT, 0)),
    ((0, LEFT), (0, RIGHT)),
    ((FAR, 0),),
    ((LEFT, LEFT), (LEFT, RIGHT), (RIGHT, LEFT), (RIGHT, RIGHT)),
    ((0, FAR),),
    ((FAR, LEFT), (FAR, RIGHT)),
    ((FAR, FAR), (LEFT, FAR), (RIGHT, FAR)),
)
DIRECT = ((0, 0), (FAR, 0), (FAR, FAR))


def dot(a, b, dims):
    return lax.dot_general(a, b, (dims, ((), ())), preferred_element_type=F32)


def body(
    ids_in, weight_in, tokens, cotangent, w_gate, w_up, w_down,
    scaled_out, layer_out,
    ids, weight, grads, tok, cot, hot, hot_t, send, slots, w_gu, w_d, acc, hid_t, hid, delta, weights,
    psend, prem, part, relay, joined, half, last, final, back, sq_send, sq_recv,
    local, z_s, z_r, a_s, a_r, b_s, b_r, d_s, d_r, p_s, p_r, q_s, q_r, j_s, j_r,
    l_s, l_r, k_s, k_r, sq_s, sq_r,
    *, experts, total,
):
    dp, z, x = lax.axis_index("dp"), lax.axis_index("expert"), lax.axis_index("ffn")
    y, c = dp // 2, dp % 2
    cap = tok.shape[1] // 2
    count = experts * cap
    units = w_gate.shape[1]
    two, four = count // 2, count // 4

    def at(v, step):
        return (v + step) % RING

    def device(x_=x, y_=y, c_=c, z_=z):
        return {"dp": y_ * 2 + c_, "expert": z_, "ffn": x_}

    def slice_of(x_, y_, c_):
        return (2 * y_ + c_) * RING + x_

    started = []

    def put(src, dst, s_sem, r_sem, dev):
        copy = pltpu.make_async_remote_copy(
            src_ref=src, dst_ref=dst, send_sem=s_sem, recv_sem=r_sem, device_id=dev, device_id_type=MESH
        )
        copy.start()
        started.append(copy)

    def arrived(dst, s_sem, r_sem):
        pltpu.make_async_remote_copy(
            src_ref=dst, dst_ref=dst, send_sem=s_sem, recv_sem=r_sem,
            device_id=device(c_=1 - c), device_id_type=MESH,
        ).wait_recv()

    def place(p, k, m):
        return (at(x, k), at(y, m)) if p == 0 else (at(x, m), at(y, k))

    def own_slice(p, k, m):
        return slice_of(*place(p, k, m), c)

    def columns(p, e):
        return pl.ds(pl.multiple_of(own_slice(p, *DIRECT[e]) * LANES, LANES), LANES)

    loads = [
        pltpu.make_async_copy(ids_in, ids, local.at[0]),
        pltpu.make_async_copy(weight_in, weight, local.at[1]),
    ]
    for e in range(len(DIRECT)):
        loads.append(pltpu.make_async_copy(tokens.at[:, columns(0, e)], tok.at[e], local.at[2 + 2 * e]))
        loads.append(pltpu.make_async_copy(cotangent.at[:, columns(1, e)], cot.at[e], local.at[3 + 2 * e]))
    loads += [
        pltpu.make_async_copy(w_gate.at[0], w_gu.at[pl.ds(0, units)], local.at[8]),
        pltpu.make_async_copy(w_up.at[0], w_gu.at[pl.ds(units, units)], local.at[9]),
        pltpu.make_async_copy(w_down.at[0], w_d.at[pl.ds(0, units)], local.at[10]),
    ]
    for load in loads[:8]:
        load.start()

    peers = [device(c_=1 - c)]
    peers += [device(x_=at(x, s)) for s in (1, 2, 3)] + [device(y_=at(y, s)) for s in (1, 2, 3)]
    peers += [device(z_=(z + j) % experts) for j in range(1, experts)]
    barrier = pltpu.get_barrier_semaphore()
    for peer in peers:
        pl.semaphore_signal(barrier, inc=1, device_id=peer, device_id_type=MESH)

    for load in loads[:2]:
        load.wait()
    rows = tok.shape[1]
    names = lax.broadcasted_iota(jnp.int32, (experts, rows), 0)
    chosen = [names == ids[k : k + 1, :] for k in (0, 1)]
    per_token = (chosen[0].astype(F32) + chosen[1].astype(F32)).astype(BF)
    before = (
        lax.broadcasted_iota(jnp.int32, (rows, rows), 0) < lax.broadcasted_iota(jnp.int32, (rows, rows), 1)
    ).astype(F32).astype(BF)
    earlier = dot(per_token, before, ((1,), (0,)))
    numbers = lax.broadcasted_iota(jnp.int32, (count, rows), 0).astype(F32)
    for k in (0, 1):
        position = jnp.sum(jnp.where(chosen[k], earlier, 0.0), axis=0, keepdims=True)
        slot = ids[k : k + 1, :].astype(F32) * float(cap) + position
        hot[k] = (numbers == slot).astype(F32).astype(BF)

    for load in loads[2:8]:
        load.wait()
    for load in loads[8:]:
        load.start()
    own_rows = pl.ds(pl.multiple_of(z * cap, cap), cap)
    either = hot[0] + hot[1]
    for k in (0, 1):
        weights[k] = jnp.broadcast_to(weight[k : k + 1, :], (LANES, rows)).T

    def exchange(p, e):
        if p == 0:
            send[p, e] = dot(either, tok[e], ((1,), (0,))).astype(BF)
        else:
            wide = cot[e].astype(F32)
            send[p, e] = sum(dot(hot[k], (weights[k] * wide).astype(BF), ((1,), (0,))) for k in (0, 1)).astype(BF)
        if p == 0 and e == 0:
            pl.semaphore_wait(barrier, len(peers))
        s = own_slice(p, *DIRECT[e])
        for j in sorted(range(1, experts), key=lambda j: -min(j, experts - j)):
            to = (z + j) % experts
            to_rows = pl.ds(pl.multiple_of(to * cap, cap), cap)
            put(
                send.at[p, e, to_rows], slots.at[p, s, own_rows],
                z_s.at[p, e, j - 1], z_r.at[p, e, j - 1], device(z_=to),
            )
        slots[p, s, own_rows, :] = send[p, e, own_rows, :]

    for e in range(len(DIRECT)):
        for p in (0, 1):
            exchange(p, e)
    acc[...] = jnp.zeros_like(acc)
    pad = w_d.shape[0] - units
    if pad:
        w_d[pl.ds(units, pad), :] = jnp.zeros((pad, w_d.shape[1]), BF)
        hid_t[pl.ds(units, pad), :] = jnp.zeros((pad, count), BF)
    for k in (0, 1):
        hot_t[k] = hot[k].astype(F32).T.astype(BF)
    for load in loads[8:]:
        load.wait()

    def await_tokens(p, e):
        for j in range(1, experts):
            source = (z + experts - j) % experts
            from_rows = pl.ds(pl.multiple_of(source * cap, cap), cap)
            arrived(slots.at[p, own_slice(p, *DIRECT[e]), from_rows], z_s.at[p, e, j - 1], z_r.at[p, e, j - 1])

    def along(p, stage, step):
        return device(x_=at(x, step)) if (p == 0) == (stage == 0) else device(y_=at(y, step))

    def whole(p, s):
        return slots.at[p, s]

    def part_of(p, s, h):
        return slots.at[p, s, pl.ds(h * two, two)]

    def both_ways(p, stage, s, s_sem, r_sem):
        for n, step in ((0, LEFT), (1, RIGHT)):
            put(whole(p, s), whole(p, s), s_sem(n), r_sem(n), along(p, stage, step))

    def onward(p, stage, s, step, s_sem, r_sem):
        n, h, to = (3, 0, RIGHT) if step == LEFT else (2, 1, LEFT)
        ref = part_of(p, s, h)
        put(ref, ref, s_sem(n), r_sem(n), along(p, stage, to))

    def sem_a(p):
        return (lambda n: a_s.at[p, n]), (lambda n: a_r.at[p, n])

    def sem_b(p, k):
        return (lambda n: b_s.at[p, k, n]), (lambda n: b_r.at[p, k, n])

    def await_slice(p, k, m):
        if (k, m) in DIRECT:
            await_tokens(p, DIRECT.index((k, m)))
            return
        s = own_slice(p, k, m)
        step, (s_sem, r_sem) = (k, sem_a(p)) if m == 0 else (m, sem_b(p, k))
        if step == LEFT:
            arrived(whole(p, s), s_sem(1), r_sem(1))
        elif step == RIGHT:
            arrived(whole(p, s), s_sem(0), r_sem(0))
        else:
            arrived(part_of(p, s, 0), s_sem(3), r_sem(3))
            arrived(part_of(p, s, 1), s_sem(2), r_sem(2))

    def accumulate(p, k, m):
        x_, y_ = place(p, k, m)
        pair = [slice_of(x_, y_, e) for e in (0, 1)]
        cols = [pl.ds(pl.multiple_of(s * LANES, LANES), LANES) for s in pair]
        right = jnp.concatenate([slots[p, s] for s in pair], axis=1)
        if p == 0:
            left = jnp.concatenate([w_gu[:, d] for d in cols], axis=1)
            acc[pl.ds(0, 2 * units), :] += dot(left, right, ((1,), (1,)))
        else:
            left = jnp.concatenate([w_d[pl.ds(0, units), d] for d in cols], axis=1)
            acc[pl.ds(2 * units, units), :] += dot(left, right, ((1,), (1,)))

    def finish(event, parts=(0, 1)):
        for k, m in event:
            for p in parts:
                x_, y_ = place(p, k, m)
                arrived(whole(p, slice_of(x_, y_, 1 - c)), d_s.at[p, k, m], d_r.at[p, k, m])
        for k, m in event:
            for p in parts:
                accumulate(p, k, m)

    def take(p, k, m):
        await_slice(p, k, m)
        s = own_slice(p, k, m)
        if m == 0:
            if k == 0:
                both_ways(p, 0, s, *sem_a(p))
        elif m != FAR and k != FAR:
            onward(p, 1, s, m, *sem_b(p, k))

    def pass_on(p, k, m):
        s = own_slice(p, k, m)
        if m == 0:
            both_ways(p, 1, s, *sem_b(p, k))
        put(whole(p, s), whole(p, s), d_s.at[p, k, m], d_r.at[p, k, m], device(c_=1 - c))

    for p in (0, 1):
        take(p, 0, 0)
        pass_on(p, 0, 0)
    previous = EVENTS[0]
    for event in EVENTS[1:]:
        for k, m in event:
            for p in (0, 1):
                take(p, k, m)
        for k, m in event:
            for p in (0, 1):
                pass_on(p, k, m)
        finish(previous)
        previous = event
    finish(previous, (0,))

    block = BLOCK

    def activate(i, carry):
        r = pl.multiple_of(i * block, block)
        gate = acc[pl.ds(r, block), :]
        up = acc[pl.ds(units + r, block), :]
        s = jax.nn.sigmoid(gate)
        active = gate * s
        hid_t[pl.ds(r, block), :] = (active * up).astype(BF)
        acc[pl.ds(r, block), :] = up * (s * (1.0 + gate * (1.0 - s)))
        acc[pl.ds(units + r, block), :] = active
        return carry

    lax.fori_loop(0, units // block, activate, 0)
    for i in range(hid_t.shape[0] // LANES):
        r = pl.ds(i * LANES, LANES)
        hid[:, r] = hid_t[r, :].astype(F32).T.astype(BF)

    width = RING * LANES

    def terms(y_, c_):
        cols = pl.ds(pl.multiple_of((2 * y_ + c_) * width, width), width)
        return dot(hid[...], w_d[:, cols], ((1,), (0,)))

    for i in range(RING):
        t = terms(i, 1 - c)
        for n in range(RING):
            psend[i, n] = t[:, n * LANES : (n + 1) * LANES].astype(BF)
        put(psend.at[i], prem.at[i], p_s.at[i], p_r.at[i], device(c_=1 - c))
    for i in range(RING):
        t = terms(i, c)
        arrived(prem.at[i], p_s.at[i], p_r.at[i])
        for n in range(RING):
            part[i, n] = (t[:, n * LANES : (n + 1) * LANES] + prem[i, n].astype(F32)).astype(BF)

    def view(h, t, start, size):
        r = pl.ds(h * two + start, size)
        return (slice(None), t, r, slice(None)) if h == 0 else (t, slice(None), r, slice(None))

    first = [x, y]
    second = [y, x]

    def hop(h, stage, step):
        return device(x_=at(x, step)) if (h == 0) == (stage == 0) else device(y_=at(y, step))

    group, piece = two // 2, two // 4

    def term(h, t, r, n):
        return part.at[view(h, t, r * group + n * piece, piece)]

    def box(ref, h, side, r, n):
        return ref.at[h, side, :, pl.ds(r * group + n * piece, piece)]

    for r in (0, 1):
        for h in (0, 1):
            for n, step in ((0, RIGHT), (1, LEFT)):
                put(
                    term(h, at(first[h], FAR), r, n), relay.at[h, r, n],
                    q_s.at[h, r, n], q_r.at[h, r, n], hop(h, 0, step),
                )
        for h in (0, 1):
            for n, step in ((0, RIGHT), (1, LEFT)):
                put(
                    term(h, at(first[h], step), r, 1 - n), box(joined, h, n, r, 1 - n),
                    j_s.at[h, r, n, 0], j_r.at[h, r, n, 0], hop(h, 0, step),
                )
    finish(EVENTS[-1], (1,))

    def deltas(i, carry):
        r = pl.multiple_of(i * block, block)
        grad = acc[pl.ds(2 * units + r, block), :]
        delta[pl.ds(r, block), :] = (grad * acc[pl.ds(r, block), :]).astype(BF)
        delta[pl.ds(units + r, block), :] = (grad * acc[pl.ds(units + r, block), :]).astype(BF)
        return carry

    lax.fori_loop(0, units // block, deltas, 0)

    def gradients(i, squares):
        pair = [2 * i, 2 * i + 1]
        cols = pl.ds(pl.multiple_of(i * 2 * LANES, 2 * LANES), 2 * LANES)
        xs = jnp.concatenate([slots[0, s] for s in pair], axis=1)
        gs = jnp.concatenate([slots[1, s] for s in pair], axis=1)
        g = dot(delta[...], xs, ((1,), (0,)))
        grads[pl.ds(0, 2 * units), cols] = g
        squares += jnp.sum((g * g).reshape(2 * units // 8, 8, 2 * LANES), axis=0)
        g = dot(hid_t[pl.ds(0, units), :], gs, ((1,), (0,)))
        grads[pl.ds(2 * units, units), cols] = g
        return squares + jnp.sum((g * g).reshape(units // 8, 8, 2 * LANES), axis=0)

    def pass_terms(r):
        for h in (0, 1):
            for n, step in ((0, RIGHT), (1, LEFT)):
                arrived(relay.at[h, r, n], q_s.at[h, r, n], q_r.at[h, r, n])
                ref = term(h, at(first[h], step), r, n)
                ref[...] = (ref[...].astype(F32) + relay[h, r, n].astype(F32)).astype(BF)
                put(ref, box(joined, h, n, r, n), j_s.at[h, r, n, 1], j_r.at[h, r, n, 1], hop(h, 0, step))

    def across(r):
        for h in (0, 1):
            for n in (0, 1):
                arrived(box(joined, h, n, r, 1 - n), j_s.at[h, r, n, 0], j_r.at[h, r, n, 0])
                arrived(box(joined, h, n, r, n), j_s.at[h, r, n, 1], j_r.at[h, r, n, 1])
            v = pl.ds(r * group, group)
            half[h, :, v, :] = (
                part[view(h, first[h], r * group, group)].astype(F32)
                + joined[h, 0, :, v, :].astype(F32) + joined[h, 1, :, v, :].astype(F32)
            ).astype(BF)
            for j in (1, 2, 3):
                put(
                    half.at[h, at(second[h], j), v], last.at[h, j - 1, v],
                    l_s.at[h, r, j - 1], l_r.at[h, r, j - 1], hop(h, 1, j),
                )

    blocks = experts // 4
    place_of = (z % (2 * blocks)) // blocks * 2 * blocks + z // (2 * blocks) * blocks + z % blocks

    def give_back(r):
        for h in (0, 1):
            v = pl.ds(r * group, group)
            summed = half[h, second[h], v, :].astype(F32)
            for j in (1, 2, 3):
                arrived(last.at[h, j - 1, v], l_s.at[h, r, j - 1], l_r.at[h, r, j - 1])
                summed = summed + last[h, j - 1, v, :].astype(F32)
            final[pl.ds(h * two + r * group, group), :] = summed.astype(BF)
        for n in range(2 * blocks - 1) if r == 0 else range(2 * blocks - 1, experts - 1):
            i = n + jnp.where(n >= place_of, 1, 0)
            to = (i // blocks) % 2 * 2 * blocks + i // (2 * blocks) * blocks + i % blocks
            to_rows = pl.ds(pl.multiple_of(to * cap, cap), cap)
            put(final.at[to_rows], back.at[own_rows], k_s.at[n], k_r.at[z], device(z_=to))

    def share(stage, value, devices, base):
        sq_send[stage] = value
        for n, dev in enumerate(devices):
            put(sq_send.at[stage], sq_recv.at[base + n], sq_s.at[base + n], sq_r.at[base + n], dev)

    def gathered(value, base, n):
        for i in range(base, base + n):
            arrived(sq_recv.at[i], sq_s.at[i], sq_r.at[i])
            value = value + sq_recv[i]
        return value

    pairs = slots.shape[1] // 2
    squares = lax.fori_loop(0, pairs // 2, gradients, jnp.zeros((8, 2 * LANES), F32))
    pass_terms(0)
    squares = lax.fori_loop(pairs // 2, pairs, gradients, squares)
    value = squares[:, :LANES] + squares[:, LANES:]
    share(0, value, [device(c_=1 - c)], 0)
    value = gathered(value, 0, 1)
    share(1, value, [device(x_=at(x, s)) for s in (1, 2, 3)], 1)
    pass_terms(1)
    across(0)
    value = gathered(value, 1, 3)
    share(2, value, [device(y_=at(y, s)) for s in (1, 2, 3)], 4)
    across(1)
    value = gathered(value, 4, 3)
    share(3, value, [device(z_=(z + j) % experts) for j in range(1, experts)], 7)
    give_back(0)
    give_back(1)
    back[own_rows, :] = final[own_rows, :]
    value = gathered(value, 7, experts - 1)
    inv = lax.rsqrt(jnp.sum(value, keepdims=True) / total + 1e-06)

    def scale(i, carry):
        r = pl.ds(pl.multiple_of(i * block, block), block)
        scaled_out[r, :] = (grads[r, :] * inv).astype(BF)
        return carry

    lax.fori_loop(0, 3 * units // block, scale, 0)
    for j in range(1, experts):
        source = (z + experts - j) % experts
        from_rows = pl.ds(pl.multiple_of(source * cap, cap), cap)
        arrived(back.at[from_rows], k_s.at[0], k_r.at[source])
    picked = [dot(hot_t[k], back[...], ((1,), (0,))) for k in (0, 1)]
    layer_out[...] = (weights[0] * picked[0] + weights[1] * picked[1]).astype(BF)
    for copy in started:
        copy.wait_send()


def copy_body(scaled, layer, gate_out, up_out, down_out, layer_out, sems):
    units = gate_out.shape[0]
    copies = [
        pltpu.make_async_copy(scaled.at[pl.ds(n * units, units)], out, sems.at[n])
        for n, out in enumerate((gate_out, up_out, down_out))
    ]
    for copy in copies:
        copy.start()
    layer_out[...] = layer[...]
    for copy in copies:
        copy.wait()


def solution(mesh):
    experts = mesh.shape["expert"]
    groups = mesh.shape["dp"] * mesh.shape["ffn"]

    def on_device(tokens, expert_ids, route_weight, cotangent, w_gate, w_up, w_down):
        rows, features = tokens.shape
        units = w_gate.shape[1]
        padded = -(-units // LANES) * LANES
        count = experts * rows // 2
        two, four = count // 2, count // 4
        total = 3.0 * experts * units * groups * features
        vmem, anywhere = pl.BlockSpec(memory_space=pltpu.VMEM), pl.BlockSpec(memory_space=pltpu.HBM)
        dma = pltpu.SemaphoreType.DMA
        scaled, layer = pl.pallas_call(
            functools.partial(body, experts=experts, total=total),
            out_shape=[
                jax.ShapeDtypeStruct((3 * units, features), BF),
                jax.ShapeDtypeStruct((rows, LANES), BF),
            ],
            in_specs=[anywhere] * 7,
            out_specs=[vmem] * 2,
            scratch_shapes=[
                pltpu.VMEM((2, rows), jnp.int32),
                pltpu.VMEM((2, rows), F32),
                pltpu.VMEM((3 * units, features), F32),
                pltpu.VMEM((len(DIRECT), rows, LANES), BF),
                pltpu.VMEM((len(DIRECT), rows, LANES), BF),
                pltpu.VMEM((2, count, rows), BF),
                pltpu.VMEM((2, rows, count), BF),
                pltpu.VMEM((2, len(DIRECT), count, LANES), BF),
                pltpu.VMEM((2, groups, count, LANES), BF),
                pltpu.VMEM((2 * units, features), BF),
                pltpu.VMEM((padded, features), BF),
                pltpu.VMEM((3 * units, count), F32),
                pltpu.VMEM((padded, count), BF),
                pltpu.VMEM((count, padded), BF),
                pltpu.VMEM((2 * units, count), BF),
                pltpu.VMEM((2, rows, LANES), F32),
                pltpu.VMEM((RING, RING, count, LANES), BF),
                pltpu.VMEM((RING, RING, count, LANES), BF),
                pltpu.VMEM((RING, RING, count, LANES), BF),
                pltpu.VMEM((2, 2, 2, RING, four // 2, LANES), BF),
                pltpu.VMEM((2, 2, RING, two, LANES), BF),
                pltpu.VMEM((2, RING, two, LANES), BF),
                pltpu.VMEM((2, 3, two, LANES), BF),
                pltpu.VMEM((count, LANES), BF),
                pltpu.VMEM((count, LANES), BF),
                pltpu.VMEM((4, 8, LANES), F32),
                pltpu.VMEM((6 + experts, 8, LANES), F32),
                dma((11,)),
                dma((2, len(DIRECT), experts - 1)), dma((2, len(DIRECT), experts - 1)),
                dma((2, 4)), dma((2, 4)),
                dma((2, RING, 4)), dma((2, RING, 4)),
                dma((2, RING, RING)), dma((2, RING, RING)),
                dma((RING,)), dma((RING,)),
                dma((2, 2, 2)), dma((2, 2, 2)),
                dma((2, 2, 2, 2)), dma((2, 2, 2, 2)),
                dma((2, 2, 3)), dma((2, 2, 3)),
                dma((experts - 1,)), dma((experts,)),
                dma((6 + experts,)), dma((6 + experts,)),
            ],
            compiler_params=pltpu.CompilerParams(
                collective_id=0, has_side_effects=True, vmem_limit_bytes=VMEM
            ),
            name="layer",
        )(
            *[
                pltpu.with_memory_space_constraint(a, pltpu.HBM)
                for a in (expert_ids.T, route_weight.T, tokens, cotangent, w_gate, w_up, w_down)
            ]
        )
        gate, up, down, layer = pl.pallas_call(
            copy_body,
            out_shape=[jax.ShapeDtypeStruct((units, features), BF)] * 3
            + [jax.ShapeDtypeStruct((rows, LANES), BF)],
            in_specs=[vmem] * 2,
            out_specs=[anywhere] * 3 + [vmem],
            scratch_shapes=[dma((3,))],
            compiler_params=pltpu.CompilerParams(vmem_limit_bytes=COPY_VMEM),
            name="copy_out",
        )(scaled, layer)
        return layer, gate[None], up[None], down[None]

    token, hidden = P("expert", None), P("expert", ("dp", "ffn"), None)
    return jax.shard_map(
        on_device,
        mesh=mesh,
        in_specs=(token, token, token, token, hidden, hidden, hidden),
        out_specs=(P("expert", ("dp", "ffn")), hidden, hidden, hidden),
        check_vma=False,
    )
```

```python
import functools

import jax
import jax.numpy as jnp
from jax import lax
from jax.experimental import pallas as pl
from jax.experimental.pallas import tpu as pltpu
from jax.sharding import PartitionSpec as P

MESH = pl.DeviceIdType.MESH
BF = jnp.bfloat16
F32 = jnp.float32
LANES = 128
BLOCK = 32
VMEM = 46 * 1024 * 1024
COPY_VMEM = 4 * 1024 * 1024
RING = 4
LEFT, RIGHT, FAR = 3, 1, 2
EVENTS = (
    ((0, 0),),
    ((LEFT, 0), (RIGHT, 0)),
    ((0, LEFT), (0, RIGHT)),
    ((FAR, 0),),
    ((LEFT, LEFT), (LEFT, RIGHT), (RIGHT, LEFT), (RIGHT, RIGHT)),
    ((0, FAR), (FAR, FAR)),
    ((FAR, LEFT), (FAR, RIGHT)),
    ((LEFT, FAR), (RIGHT, FAR)),
)
DIRECT = ((0, 0), (FAR, 0), (FAR, FAR))


def dot(a, b, dims):
    return lax.dot_general(a, b, (dims, ((), ())), preferred_element_type=F32)


def body(
    ids_in, weight_in, tokens, cotangent, w_gate, w_up, w_down,
    scaled_out, back, hot_t, weights,
    ids, weight, grads, tok, cot, hot, send, slots, w_gu, w_d, acc, hid_t, hid, delta,
    psend, prem, part, relay, joined, half, last, final, sq_send, sq_recv,
    local, z_s, z_r, a_s, a_r, b_s, b_r, d_s, d_r, p_s, p_r, q_s, q_r, j_s, j_r,
    l_s, l_r, k_s, k_r, sq_s, sq_r,
    *, experts, total,
):
    dp, z, x = lax.axis_index("dp"), lax.axis_index("expert"), lax.axis_index("ffn")
    y, c = dp // 2, dp % 2
    cap = tok.shape[1] // 2
    count = experts * cap
    units = w_gate.shape[1]
    two, four = count // 2, count // 4

    def at(v, step):
        return (v + step) % RING

    def device(x_=x, y_=y, c_=c, z_=z):
        return {"dp": y_ * 2 + c_, "expert": z_, "ffn": x_}

    def slice_of(x_, y_, c_):
        return (2 * y_ + c_) * RING + x_

    started = []

    def put(src, dst, s_sem, r_sem, dev):
        copy = pltpu.make_async_remote_copy(
            src_ref=src, dst_ref=dst, send_sem=s_sem, recv_sem=r_sem, device_id=dev, device_id_type=MESH
        )
        copy.start()
        started.append(copy)

    def arrived(dst, s_sem, r_sem):
        pltpu.make_async_remote_copy(
            src_ref=dst, dst_ref=dst, send_sem=s_sem, recv_sem=r_sem,
            device_id=device(c_=1 - c), device_id_type=MESH,
        ).wait_recv()

    def place(p, k, m):
        return (at(x, k), at(y, m)) if p == 0 else (at(x, m), at(y, k))

    def own_slice(p, k, m):
        return slice_of(*place(p, k, m), c)

    def columns(p, e):
        return pl.ds(pl.multiple_of(own_slice(p, *DIRECT[e]) * LANES, LANES), LANES)

    loads = [
        pltpu.make_async_copy(ids_in, ids, local.at[0]),
        pltpu.make_async_copy(weight_in, weight, local.at[1]),
    ]
    for e in range(len(DIRECT)):
        loads.append(pltpu.make_async_copy(tokens.at[:, columns(0, e)], tok.at[e], local.at[2 + 2 * e]))
        loads.append(pltpu.make_async_copy(cotangent.at[:, columns(1, e)], cot.at[e], local.at[3 + 2 * e]))
    loads += [
        pltpu.make_async_copy(w_gate.at[0], w_gu.at[pl.ds(0, units)], local.at[8]),
        pltpu.make_async_copy(w_up.at[0], w_gu.at[pl.ds(units, units)], local.at[9]),
        pltpu.make_async_copy(w_down.at[0], w_d.at[pl.ds(0, units)], local.at[10]),
    ]
    for load in loads[:8]:
        load.start()

    peers = [device(c_=1 - c)]
    peers += [device(x_=at(x, s)) for s in (1, 2, 3)] + [device(y_=at(y, s)) for s in (1, 2, 3)]
    peers += [device(z_=(z + j) % experts) for j in range(1, experts)]
    barrier = pltpu.get_barrier_semaphore()
    for peer in peers:
        pl.semaphore_signal(barrier, inc=1, device_id=peer, device_id_type=MESH)

    for load in loads[:2]:
        load.wait()
    rows = tok.shape[1]
    names = lax.broadcasted_iota(jnp.int32, (experts, rows), 0)
    chosen = [names == ids[k : k + 1, :] for k in (0, 1)]
    per_token = (chosen[0].astype(F32) + chosen[1].astype(F32)).astype(BF)
    before = (
        lax.broadcasted_iota(jnp.int32, (rows, rows), 0) < lax.broadcasted_iota(jnp.int32, (rows, rows), 1)
    ).astype(F32).astype(BF)
    earlier = dot(per_token, before, ((1,), (0,)))
    numbers = lax.broadcasted_iota(jnp.int32, (count, rows), 0).astype(F32)
    for k in (0, 1):
        position = jnp.sum(jnp.where(chosen[k], earlier, 0.0), axis=0, keepdims=True)
        slot = ids[k : k + 1, :].astype(F32) * float(cap) + position
        hot[k] = (numbers == slot).astype(F32).astype(BF)

    for load in loads[2:8]:
        load.wait()
    for load in loads[8:]:
        load.start()
    own_rows = pl.ds(pl.multiple_of(z * cap, cap), cap)
    either = hot[0] + hot[1]
    for k in (0, 1):
        weights[k] = jnp.broadcast_to(weight[k : k + 1, :], (LANES, rows)).T

    def exchange(p, e):
        if p == 0:
            send[p, e] = dot(either, tok[e], ((1,), (0,))).astype(BF)
        else:
            wide = cot[e].astype(F32)
            send[p, e] = sum(dot(hot[k], (weights[k] * wide).astype(BF), ((1,), (0,))) for k in (0, 1)).astype(BF)
        if p == 0 and e == 0:
            pl.semaphore_wait(barrier, len(peers))
        s = own_slice(p, *DIRECT[e])
        for j in sorted(range(1, experts), key=lambda j: -min(j, experts - j)):
            to = (z + j) % experts
            to_rows = pl.ds(pl.multiple_of(to * cap, cap), cap)
            put(
                send.at[p, e, to_rows], slots.at[p, s, own_rows],
                z_s.at[p, e, j - 1], z_r.at[p, e, j - 1], device(z_=to),
            )
        slots[p, s, own_rows, :] = send[p, e, own_rows, :]

    for e in range(len(DIRECT)):
        for p in (0, 1):
            exchange(p, e)
    acc[...] = jnp.zeros_like(acc)
    pad = w_d.shape[0] - units
    if pad:
        w_d[pl.ds(units, pad), :] = jnp.zeros((pad, w_d.shape[1]), BF)
        hid_t[pl.ds(units, pad), :] = jnp.zeros((pad, count), BF)
    for k in (0, 1):
        hot_t[k] = hot[k].astype(F32).T.astype(BF)
    for load in loads[8:]:
        load.wait()

    def await_tokens(p, e):
        for j in range(1, experts):
            source = (z + experts - j) % experts
            from_rows = pl.ds(pl.multiple_of(source * cap, cap), cap)
            arrived(slots.at[p, own_slice(p, *DIRECT[e]), from_rows], z_s.at[p, e, j - 1], z_r.at[p, e, j - 1])

    def along(p, stage, step):
        return device(x_=at(x, step)) if (p == 0) == (stage == 0) else device(y_=at(y, step))

    def whole(p, s):
        return slots.at[p, s]

    def part_of(p, s, h):
        return slots.at[p, s, pl.ds(h * two, two)]

    def both_ways(p, stage, s, s_sem, r_sem):
        for n, step in ((0, LEFT), (1, RIGHT)):
            put(whole(p, s), whole(p, s), s_sem(n), r_sem(n), along(p, stage, step))

    def onward(p, stage, s, step, s_sem, r_sem):
        n, h, to = (3, 0, RIGHT) if step == LEFT else (2, 1, LEFT)
        ref = part_of(p, s, h)
        put(ref, ref, s_sem(n), r_sem(n), along(p, stage, to))

    def sem_a(p):
        return (lambda n: a_s.at[p, n]), (lambda n: a_r.at[p, n])

    def sem_b(p, k):
        return (lambda n: b_s.at[p, k, n]), (lambda n: b_r.at[p, k, n])

    def await_slice(p, k, m):
        if (k, m) in DIRECT:
            await_tokens(p, DIRECT.index((k, m)))
            return
        s = own_slice(p, k, m)
        step, (s_sem, r_sem) = (k, sem_a(p)) if m == 0 else (m, sem_b(p, k))
        if step == LEFT:
            arrived(whole(p, s), s_sem(1), r_sem(1))
        elif step == RIGHT:
            arrived(whole(p, s), s_sem(0), r_sem(0))
        else:
            arrived(part_of(p, s, 0), s_sem(3), r_sem(3))
            arrived(part_of(p, s, 1), s_sem(2), r_sem(2))

    def accumulate(p, k, m):
        x_, y_ = place(p, k, m)
        pair = [slice_of(x_, y_, e) for e in (0, 1)]
        cols = [pl.ds(pl.multiple_of(s * LANES, LANES), LANES) for s in pair]
        right = jnp.concatenate([slots[p, s] for s in pair], axis=1)
        if p == 0:
            left = jnp.concatenate([w_gu[:, d] for d in cols], axis=1)
            acc[pl.ds(0, 2 * units), :] += dot(left, right, ((1,), (1,)))
        else:
            left = jnp.concatenate([w_d[pl.ds(0, units), d] for d in cols], axis=1)
            acc[pl.ds(2 * units, units), :] += dot(left, right, ((1,), (1,)))

    def finish(event, parts=(0, 1)):
        for k, m in event:
            for p in parts:
                x_, y_ = place(p, k, m)
                arrived(whole(p, slice_of(x_, y_, 1 - c)), d_s.at[p, k, m], d_r.at[p, k, m])
        for k, m in event:
            for p in parts:
                accumulate(p, k, m)

    def take(p, k, m):
        await_slice(p, k, m)
        s = own_slice(p, k, m)
        if m == 0:
            if k == 0:
                both_ways(p, 0, s, *sem_a(p))
        elif m != FAR and k != FAR:
            onward(p, 1, s, m, *sem_b(p, k))

    def pass_on(p, k, m):
        s = own_slice(p, k, m)
        if m == 0:
            both_ways(p, 1, s, *sem_b(p, k))
        put(whole(p, s), whole(p, s), d_s.at[p, k, m], d_r.at[p, k, m], device(c_=1 - c))

    for p in (0, 1):
        take(p, 0, 0)
        pass_on(p, 0, 0)
    previous = EVENTS[0]
    for event in EVENTS[1:]:
        for k, m in event:
            for p in (0, 1):
                take(p, k, m)
        for k, m in event:
            for p in (0, 1):
                pass_on(p, k, m)
        finish(previous)
        previous = event
    finish(previous, (0,))

    block = BLOCK

    def activate(i, carry):
        r = pl.multiple_of(i * block, block)
        gate = acc[pl.ds(r, block), :]
        up = acc[pl.ds(units + r, block), :]
        s = jax.nn.sigmoid(gate)
        active = gate * s
        hid_t[pl.ds(r, block), :] = (active * up).astype(BF)
        acc[pl.ds(r, block), :] = up * (s * (1.0 + gate * (1.0 - s)))
        acc[pl.ds(units + r, block), :] = active
        return carry

    lax.fori_loop(0, units // block, activate, 0)
    for i in range(hid_t.shape[0] // LANES):
        r = pl.ds(i * LANES, LANES)
        hid[:, r] = hid_t[r, :].astype(F32).T.astype(BF)

    width = RING * LANES

    def terms(y_, c_):
        cols = pl.ds(pl.multiple_of((2 * y_ + c_) * width, width), width)
        return dot(hid[...], w_d[:, cols], ((1,), (0,)))

    for i in range(RING):
        t = terms(i, 1 - c)
        for n in range(RING):
            psend[i, n] = t[:, n * LANES : (n + 1) * LANES].astype(BF)
        put(psend.at[i], prem.at[i], p_s.at[i], p_r.at[i], device(c_=1 - c))
    for i in range(RING):
        t = terms(i, c)
        arrived(prem.at[i], p_s.at[i], p_r.at[i])
        for n in range(RING):
            part[i, n] = (t[:, n * LANES : (n + 1) * LANES] + prem[i, n].astype(F32)).astype(BF)

    def view(h, t, start, size):
        r = pl.ds(h * two + start, size)
        return (slice(None), t, r, slice(None)) if h == 0 else (t, slice(None), r, slice(None))

    first = [x, y]
    second = [y, x]

    def hop(h, stage, step):
        return device(x_=at(x, step)) if (h == 0) == (stage == 0) else device(y_=at(y, step))

    group, piece = two // 2, two // 4

    def term(h, t, r, n):
        return part.at[view(h, t, r * group + n * piece, piece)]

    def box(ref, h, side, r, n):
        return ref.at[h, side, :, pl.ds(r * group + n * piece, piece)]

    for r in (0, 1):
        for h in (0, 1):
            for n, step in ((0, RIGHT), (1, LEFT)):
                put(
                    term(h, at(first[h], FAR), r, n), relay.at[h, r, n],
                    q_s.at[h, r, n], q_r.at[h, r, n], hop(h, 0, step),
                )
        for h in (0, 1):
            for n, step in ((0, RIGHT), (1, LEFT)):
                put(
                    term(h, at(first[h], step), r, 1 - n), box(joined, h, n, r, 1 - n),
                    j_s.at[h, r, n, 0], j_r.at[h, r, n, 0], hop(h, 0, step),
                )
    finish(EVENTS[-1], (1,))

    def deltas(i, carry):
        r = pl.multiple_of(i * block, block)
        grad = acc[pl.ds(2 * units + r, block), :]
        delta[pl.ds(r, block), :] = (grad * acc[pl.ds(r, block), :]).astype(BF)
        delta[pl.ds(units + r, block), :] = (grad * acc[pl.ds(units + r, block), :]).astype(BF)
        return carry

    lax.fori_loop(0, units // block, deltas, 0)

    def gradients(i, squares):
        pair = [2 * i, 2 * i + 1]
        cols = pl.ds(pl.multiple_of(i * 2 * LANES, 2 * LANES), 2 * LANES)
        xs = jnp.concatenate([slots[0, s] for s in pair], axis=1)
        gs = jnp.concatenate([slots[1, s] for s in pair], axis=1)
        g = dot(delta[...], xs, ((1,), (0,)))
        grads[pl.ds(0, 2 * units), cols] = g
        squares += jnp.sum((g * g).reshape(2 * units // 8, 8, 2 * LANES), axis=0)
        g = dot(hid_t[pl.ds(0, units), :], gs, ((1,), (0,)))
        grads[pl.ds(2 * units, units), cols] = g
        return squares + jnp.sum((g * g).reshape(units // 8, 8, 2 * LANES), axis=0)

    def pass_terms(r):
        for h in (0, 1):
            for n, step in ((0, RIGHT), (1, LEFT)):
                arrived(relay.at[h, r, n], q_s.at[h, r, n], q_r.at[h, r, n])
                ref = term(h, at(first[h], step), r, n)
                ref[...] = (ref[...].astype(F32) + relay[h, r, n].astype(F32)).astype(BF)
                put(ref, box(joined, h, n, r, n), j_s.at[h, r, n, 1], j_r.at[h, r, n, 1], hop(h, 0, step))

    def across(r):
        for h in (0, 1):
            for n in (0, 1):
                arrived(box(joined, h, n, r, 1 - n), j_s.at[h, r, n, 0], j_r.at[h, r, n, 0])
                arrived(box(joined, h, n, r, n), j_s.at[h, r, n, 1], j_r.at[h, r, n, 1])
            v = pl.ds(r * group, group)
            half[h, :, v, :] = (
                part[view(h, first[h], r * group, group)].astype(F32)
                + joined[h, 0, :, v, :].astype(F32) + joined[h, 1, :, v, :].astype(F32)
            ).astype(BF)
            for j in (1, 2, 3):
                put(
                    half.at[h, at(second[h], j), v], last.at[h, j - 1, v],
                    l_s.at[h, r, j - 1], l_r.at[h, r, j - 1], hop(h, 1, j),
                )

    blocks = experts // 4
    place_of = (z % (2 * blocks)) // blocks * 2 * blocks + z // (2 * blocks) * blocks + z % blocks

    def give_back(r):
        for h in (0, 1):
            v = pl.ds(r * group, group)
            summed = half[h, second[h], v, :].astype(F32)
            for j in (1, 2, 3):
                arrived(last.at[h, j - 1, v], l_s.at[h, r, j - 1], l_r.at[h, r, j - 1])
                summed = summed + last[h, j - 1, v, :].astype(F32)
            final[pl.ds(h * two + r * group, group), :] = summed.astype(BF)
        for n in range(2 * blocks - 1) if r == 0 else range(2 * blocks - 1, experts - 1):
            i = n + jnp.where(n >= place_of, 1, 0)
            to = (i // blocks) % 2 * 2 * blocks + i // (2 * blocks) * blocks + i % blocks
            to_rows = pl.ds(pl.multiple_of(to * cap, cap), cap)
            put(final.at[to_rows], back.at[own_rows], k_s.at[n], k_r.at[z], device(z_=to))

    def share(stage, value, devices, base):
        sq_send[stage] = value
        for n, dev in enumerate(devices):
            put(sq_send.at[stage], sq_recv.at[base + n], sq_s.at[base + n], sq_r.at[base + n], dev)

    def gathered(value, base, n):
        for i in range(base, base + n):
            arrived(sq_recv.at[i], sq_s.at[i], sq_r.at[i])
            value = value + sq_recv[i]
        return value

    pairs = slots.shape[1] // 2
    squares = lax.fori_loop(0, 3 * pairs // 4, gradients, jnp.zeros((8, 2 * LANES), F32))
    pass_terms(0)
    squares = lax.fori_loop(3 * pairs // 4, pairs, gradients, squares)
    value = squares[:, :LANES] + squares[:, LANES:]
    share(0, value, [device(c_=1 - c)], 0)
    value = gathered(value, 0, 1)
    share(1, value, [device(x_=at(x, s)) for s in (1, 2, 3)], 1)
    pass_terms(1)
    across(0)
    value = gathered(value, 1, 3)
    share(2, value, [device(y_=at(y, s)) for s in (1, 2, 3)], 4)
    across(1)
    value = gathered(value, 4, 3)
    share(3, value, [device(z_=(z + j) % experts) for j in range(1, experts)], 7)
    give_back(0)
    give_back(1)
    back[own_rows, :] = final[own_rows, :]
    value = gathered(value, 7, experts - 1)
    inv = lax.rsqrt(jnp.sum(value, keepdims=True) / total + 1e-06)

    def scale(i, carry):
        r = pl.ds(pl.multiple_of(i * block, block), block)
        scaled_out[r, :] = (grads[r, :] * inv).astype(BF)
        return carry

    lax.fori_loop(0, 3 * units // block, scale, 0)
    for copy in started:
        copy.wait_send()
    for j in range(1, experts):
        source = (z + experts - j) % experts
        from_rows = pl.ds(pl.multiple_of(source * cap, cap), cap)
        arrived(back.at[from_rows], k_s.at[0], k_r.at[source])


def copy_body(scaled, back, hot_t, weights, gate_out, up_out, down_out, layer_out, sems):
    units = gate_out.shape[0]
    blocks = units // BLOCK
    copies = [
        pltpu.make_async_copy(
            scaled.at[pl.ds(n * units + i * BLOCK, BLOCK)], out.at[pl.ds(i * BLOCK, BLOCK)], sems.at[n * blocks + i]
        )
        for i in range(blocks) for n, out in enumerate((gate_out, up_out, down_out))
    ]
    for copy in copies:
        copy.start()
    picked = [dot(hot_t[k], back[...], ((1,), (0,))) for k in (0, 1)]
    layer_out[...] = (weights[0] * picked[0] + weights[1] * picked[1]).astype(BF)
    for copy in copies:
        copy.wait()


def solution(mesh):
    experts = mesh.shape["expert"]
    groups = mesh.shape["dp"] * mesh.shape["ffn"]

    def on_device(tokens, expert_ids, route_weight, cotangent, w_gate, w_up, w_down):
        rows, features = tokens.shape
        units = w_gate.shape[1]
        padded = -(-units // LANES) * LANES
        count = experts * rows // 2
        two, four = count // 2, count // 4
        total = 3.0 * experts * units * groups * features
        vmem, anywhere = pl.BlockSpec(memory_space=pltpu.VMEM), pl.BlockSpec(memory_space=pltpu.HBM)
        dma = pltpu.SemaphoreType.DMA
        scaled, back, hot_t, weights = pl.pallas_call(
            functools.partial(body, experts=experts, total=total),
            out_shape=[
                jax.ShapeDtypeStruct((3 * units, features), BF),
                jax.ShapeDtypeStruct((count, LANES), BF),
                jax.ShapeDtypeStruct((2, rows, count), BF),
                jax.ShapeDtypeStruct((2, rows, LANES), F32),
            ],
            in_specs=[anywhere] * 7,
            out_specs=[vmem] * 4,
            scratch_shapes=[
                pltpu.VMEM((2, rows), jnp.int32),
                pltpu.VMEM((2, rows), F32),
                pltpu.VMEM((3 * units, features), F32),
                pltpu.VMEM((len(DIRECT), rows, LANES), BF),
                pltpu.VMEM((len(DIRECT), rows, LANES), BF),
                pltpu.VMEM((2, count, rows), BF),
                pltpu.VMEM((2, len(DIRECT), count, LANES), BF),
                pltpu.VMEM((2, groups, count, LANES), BF),
                pltpu.VMEM((2 * units, features), BF),
                pltpu.VMEM((padded, features), BF),
                pltpu.VMEM((3 * units, count), F32),
                pltpu.VMEM((padded, count), BF),
                pltpu.VMEM((count, padded), BF),
                pltpu.VMEM((2 * units, count), BF),
                pltpu.VMEM((RING, RING, count, LANES), BF),
                pltpu.VMEM((RING, RING, count, LANES), BF),
                pltpu.VMEM((RING, RING, count, LANES), BF),
                pltpu.VMEM((2, 2, 2, RING, four // 2, LANES), BF),
                pltpu.VMEM((2, 2, RING, two, LANES), BF),
                pltpu.VMEM((2, RING, two, LANES), BF),
                pltpu.VMEM((2, 3, two, LANES), BF),
                pltpu.VMEM((count, LANES), BF),
                pltpu.VMEM((4, 8, LANES), F32),
                pltpu.VMEM((6 + experts, 8, LANES), F32),
                dma((11,)),
                dma((2, len(DIRECT), experts - 1)), dma((2, len(DIRECT), experts - 1)),
                dma((2, 4)), dma((2, 4)),
                dma((2, RING, 4)), dma((2, RING, 4)),
                dma((2, RING, RING)), dma((2, RING, RING)),
                dma((RING,)), dma((RING,)),
                dma((2, 2, 2)), dma((2, 2, 2)),
                dma((2, 2, 2, 2)), dma((2, 2, 2, 2)),
                dma((2, 2, 3)), dma((2, 2, 3)),
                dma((experts - 1,)), dma((experts,)),
                dma((6 + experts,)), dma((6 + experts,)),
            ],
            compiler_params=pltpu.CompilerParams(
                collective_id=0, has_side_effects=True, vmem_limit_bytes=VMEM
            ),
            name="layer",
        )(
            *[
                pltpu.with_memory_space_constraint(a, pltpu.HBM)
                for a in (expert_ids.T, route_weight.T, tokens, cotangent, w_gate, w_up, w_down)
            ]
        )
        gate, up, down, layer = pl.pallas_call(
            copy_body,
            out_shape=[jax.ShapeDtypeStruct((units, features), BF)] * 3
            + [jax.ShapeDtypeStruct((rows, LANES), BF)],
            in_specs=[vmem] * 4,
            out_specs=[anywhere] * 3 + [vmem],
            scratch_shapes=[dma((3 * (units // BLOCK),))],
            compiler_params=pltpu.CompilerParams(vmem_limit_bytes=COPY_VMEM),
            name="copy_out",
        )(scaled, back, hot_t, weights)
        return layer, gate[None], up[None], down[None]

    token, hidden = P("expert", None), P("expert", ("dp", "ffn"), None)
    return jax.shard_map(
        on_device,
        mesh=mesh,
        in_specs=(token, token, token, token, hidden, hidden, hidden),
        out_specs=(P("expert", ("dp", "ffn")), hidden, hidden, hidden),
        check_vma=False,
    )
```

```python
import functools

import jax
import jax.numpy as jnp
from jax import lax
from jax.experimental import pallas as pl
from jax.experimental.pallas import tpu as pltpu
from jax.sharding import PartitionSpec as P

MESH = pl.DeviceIdType.MESH
BF = jnp.bfloat16
F32 = jnp.float32
LANES = 128
BLOCK = 32
VMEM = 46 * 1024 * 1024
COPY_VMEM = 4 * 1024 * 1024
RING = 4
LEFT, RIGHT, FAR = 3, 1, 2
EVENTS = (
    ((0, 0),),
    ((LEFT, 0), (RIGHT, 0)),
    ((0, LEFT), (0, RIGHT)),
    ((FAR, 0),),
    ((LEFT, LEFT), (LEFT, RIGHT), (RIGHT, LEFT), (RIGHT, RIGHT)),
    ((0, FAR), (FAR, FAR)),
    ((FAR, LEFT), (FAR, RIGHT)),
    ((LEFT, FAR), (RIGHT, FAR)),
)
DIRECT = ((0, 0), (FAR, 0), (FAR, FAR))


def dot(a, b, dims):
    return lax.dot_general(a, b, (dims, ((), ())), preferred_element_type=F32)


def body(
    ids_in, weight_in, tokens, cotangent, w_gate, w_up, w_down,
    scaled_out, back, hot_t, weights,
    ids, weight, grads, tok, cot, hot, send, slots, w_gu, w_d, acc, hid_t, hid, delta,
    psend, prem, part, relay, joined, half, last, final, sq_send, sq_recv,
    local, z_s, z_r, a_s, a_r, b_s, b_r, d_s, d_r, p_s, p_r, q_s, q_r, j_s, j_r,
    l_s, l_r, k_s, k_r, sq_s, sq_r,
    *, experts, total,
):
    dp, z, x = lax.axis_index("dp"), lax.axis_index("expert"), lax.axis_index("ffn")
    y, c = dp // 2, dp % 2
    cap = tok.shape[1] // 2
    count = experts * cap
    units = w_gate.shape[1]
    two, four = count // 2, count // 4

    def at(v, step):
        return (v + step) % RING

    def device(x_=x, y_=y, c_=c, z_=z):
        return {"dp": y_ * 2 + c_, "expert": z_, "ffn": x_}

    def slice_of(x_, y_, c_):
        return (2 * y_ + c_) * RING + x_

    started = []

    def put(src, dst, s_sem, r_sem, dev):
        copy = pltpu.make_async_remote_copy(
            src_ref=src, dst_ref=dst, send_sem=s_sem, recv_sem=r_sem, device_id=dev, device_id_type=MESH
        )
        copy.start()
        started.append(copy)

    def arrived(dst, s_sem, r_sem):
        pltpu.make_async_remote_copy(
            src_ref=dst, dst_ref=dst, send_sem=s_sem, recv_sem=r_sem,
            device_id=device(c_=1 - c), device_id_type=MESH,
        ).wait_recv()

    def place(p, k, m):
        return (at(x, k), at(y, m)) if p == 0 else (at(x, m), at(y, k))

    def own_slice(p, k, m):
        return slice_of(*place(p, k, m), c)

    def columns(p, e):
        return pl.ds(pl.multiple_of(own_slice(p, *DIRECT[e]) * LANES, LANES), LANES)

    loads = [
        pltpu.make_async_copy(ids_in, ids, local.at[0]),
        pltpu.make_async_copy(weight_in, weight, local.at[1]),
    ]
    for e in range(len(DIRECT)):
        loads.append(pltpu.make_async_copy(tokens.at[:, columns(0, e)], tok.at[e], local.at[2 + 2 * e]))
        loads.append(pltpu.make_async_copy(cotangent.at[:, columns(1, e)], cot.at[e], local.at[3 + 2 * e]))
    loads += [
        pltpu.make_async_copy(w_gate.at[0], w_gu.at[pl.ds(0, units)], local.at[8]),
        pltpu.make_async_copy(w_up.at[0], w_gu.at[pl.ds(units, units)], local.at[9]),
        pltpu.make_async_copy(w_down.at[0], w_d.at[pl.ds(0, units)], local.at[10]),
    ]
    for load in loads[:8]:
        load.start()

    peers = [device(c_=1 - c)]
    peers += [device(x_=at(x, s)) for s in (1, 2, 3)] + [device(y_=at(y, s)) for s in (1, 2, 3)]
    peers += [device(z_=(z + j) % experts) for j in range(1, experts)]
    barrier = pltpu.get_barrier_semaphore()
    for peer in peers:
        pl.semaphore_signal(barrier, inc=1, device_id=peer, device_id_type=MESH)

    for load in loads[:2]:
        load.wait()
    rows = tok.shape[1]
    names = lax.broadcasted_iota(jnp.int32, (experts, rows), 0)
    chosen = [names == ids[k : k + 1, :] for k in (0, 1)]
    per_token = (chosen[0].astype(F32) + chosen[1].astype(F32)).astype(BF)
    before = (
        lax.broadcasted_iota(jnp.int32, (rows, rows), 0) < lax.broadcasted_iota(jnp.int32, (rows, rows), 1)
    ).astype(F32).astype(BF)
    earlier = dot(per_token, before, ((1,), (0,)))
    numbers = lax.broadcasted_iota(jnp.int32, (count, rows), 0).astype(F32)
    for k in (0, 1):
        position = jnp.sum(jnp.where(chosen[k], earlier, 0.0), axis=0, keepdims=True)
        slot = ids[k : k + 1, :].astype(F32) * float(cap) + position
        hot[k] = (numbers == slot).astype(F32).astype(BF)

    loads[2].wait()
    own_rows = pl.ds(pl.multiple_of(z * cap, cap), cap)
    either = hot[0] + hot[1]

    def exchange(p, e):
        if p == 0:
            send[p, e] = dot(either, tok[e], ((1,), (0,))).astype(BF)
        else:
            wide = cot[e].astype(F32)
            send[p, e] = sum(dot(hot[k], (weights[k] * wide).astype(BF), ((1,), (0,))) for k in (0, 1)).astype(BF)
        if p == 0 and e == 0:
            pl.semaphore_wait(barrier, len(peers))
        s = own_slice(p, *DIRECT[e])
        for j in sorted(range(1, experts), key=lambda j: -min(j, experts - j)):
            to = (z + j) % experts
            to_rows = pl.ds(pl.multiple_of(to * cap, cap), cap)
            put(
                send.at[p, e, to_rows], slots.at[p, s, own_rows],
                z_s.at[p, e, j - 1], z_r.at[p, e, j - 1], device(z_=to),
            )
        slots[p, s, own_rows, :] = send[p, e, own_rows, :]

    exchange(0, 0)
    for load in loads[3:8]:
        load.wait()
    for load in loads[8:]:
        load.start()
    for k in (0, 1):
        weights[k] = jnp.broadcast_to(weight[k : k + 1, :], (LANES, rows)).T
    for e in range(len(DIRECT)):
        for p in (0, 1):
            if (p, e) != (0, 0):
                exchange(p, e)
    acc[...] = jnp.zeros_like(acc)
    pad = w_d.shape[0] - units
    if pad:
        w_d[pl.ds(units, pad), :] = jnp.zeros((pad, w_d.shape[1]), BF)
        hid_t[pl.ds(units, pad), :] = jnp.zeros((pad, count), BF)
    for k in (0, 1):
        hot_t[k] = hot[k].astype(F32).T.astype(BF)
    for load in loads[8:]:
        load.wait()

    def await_tokens(p, e):
        for j in range(1, experts):
            source = (z + experts - j) % experts
            from_rows = pl.ds(pl.multiple_of(source * cap, cap), cap)
            arrived(slots.at[p, own_slice(p, *DIRECT[e]), from_rows], z_s.at[p, e, j - 1], z_r.at[p, e, j - 1])

    def along(p, stage, step):
        return device(x_=at(x, step)) if (p == 0) == (stage == 0) else device(y_=at(y, step))

    def whole(p, s):
        return slots.at[p, s]

    def part_of(p, s, h):
        return slots.at[p, s, pl.ds(h * two, two)]

    def both_ways(p, stage, s, s_sem, r_sem):
        for n, step in ((0, LEFT), (1, RIGHT)):
            put(whole(p, s), whole(p, s), s_sem(n), r_sem(n), along(p, stage, step))

    def onward(p, stage, s, step, s_sem, r_sem):
        n, h, to = (3, 0, RIGHT) if step == LEFT else (2, 1, LEFT)
        ref = part_of(p, s, h)
        put(ref, ref, s_sem(n), r_sem(n), along(p, stage, to))

    def sem_a(p):
        return (lambda n: a_s.at[p, n]), (lambda n: a_r.at[p, n])

    def sem_b(p, k):
        return (lambda n: b_s.at[p, k, n]), (lambda n: b_r.at[p, k, n])

    def await_slice(p, k, m):
        if (k, m) in DIRECT:
            await_tokens(p, DIRECT.index((k, m)))
            return
        s = own_slice(p, k, m)
        step, (s_sem, r_sem) = (k, sem_a(p)) if m == 0 else (m, sem_b(p, k))
        if step == LEFT:
            arrived(whole(p, s), s_sem(1), r_sem(1))
        elif step == RIGHT:
            arrived(whole(p, s), s_sem(0), r_sem(0))
        else:
            arrived(part_of(p, s, 0), s_sem(3), r_sem(3))
            arrived(part_of(p, s, 1), s_sem(2), r_sem(2))

    def accumulate(p, k, m):
        x_, y_ = place(p, k, m)
        pair = [slice_of(x_, y_, e) for e in (0, 1)]
        cols = [pl.ds(pl.multiple_of(s * LANES, LANES), LANES) for s in pair]
        right = jnp.concatenate([slots[p, s] for s in pair], axis=1)
        if p == 0:
            left = jnp.concatenate([w_gu[:, d] for d in cols], axis=1)
            acc[pl.ds(0, 2 * units), :] += dot(left, right, ((1,), (1,)))
        else:
            left = jnp.concatenate([w_d[pl.ds(0, units), d] for d in cols], axis=1)
            acc[pl.ds(2 * units, units), :] += dot(left, right, ((1,), (1,)))

    def finish(event, parts=(0, 1)):
        for k, m in event:
            for p in parts:
                x_, y_ = place(p, k, m)
                arrived(whole(p, slice_of(x_, y_, 1 - c)), d_s.at[p, k, m], d_r.at[p, k, m])
        for k, m in event:
            for p in parts:
                accumulate(p, k, m)

    def take(p, k, m):
        await_slice(p, k, m)
        s = own_slice(p, k, m)
        if m == 0:
            if k == 0:
                both_ways(p, 0, s, *sem_a(p))
        elif m != FAR and k != FAR:
            onward(p, 1, s, m, *sem_b(p, k))

    def pass_on(p, k, m):
        s = own_slice(p, k, m)
        if m == 0:
            both_ways(p, 1, s, *sem_b(p, k))
        put(whole(p, s), whole(p, s), d_s.at[p, k, m], d_r.at[p, k, m], device(c_=1 - c))

    for p in (0, 1):
        take(p, 0, 0)
        pass_on(p, 0, 0)
    previous = EVENTS[0]
    for event in EVENTS[1:]:
        for k, m in event:
            for p in (0, 1):
                take(p, k, m)
        for k, m in event:
            for p in (0, 1):
                pass_on(p, k, m)
        finish(previous)
        previous = event
    finish(previous, (0,))

    block = BLOCK

    def activate(i, carry):
        r = pl.multiple_of(i * block, block)
        gate = acc[pl.ds(r, block), :]
        up = acc[pl.ds(units + r, block), :]
        s = jax.nn.sigmoid(gate)
        active = gate * s
        hid_t[pl.ds(r, block), :] = (active * up).astype(BF)
        acc[pl.ds(r, block), :] = up * (s * (1.0 + gate * (1.0 - s)))
        acc[pl.ds(units + r, block), :] = active
        return carry

    lax.fori_loop(0, units // block, activate, 0)
    for i in range(hid_t.shape[0] // LANES):
        r = pl.ds(i * LANES, LANES)
        hid[:, r] = hid_t[r, :].astype(F32).T.astype(BF)

    width = RING * LANES

    def terms(y_, c_):
        cols = pl.ds(pl.multiple_of((2 * y_ + c_) * width, width), width)
        return dot(hid[...], w_d[:, cols], ((1,), (0,)))

    for i in range(RING):
        t = terms(i, 1 - c)
        for n in range(RING):
            psend[i, n] = t[:, n * LANES : (n + 1) * LANES].astype(BF)
        put(psend.at[i], prem.at[i], p_s.at[i], p_r.at[i], device(c_=1 - c))
    for i in range(RING):
        t = terms(i, c)
        arrived(prem.at[i], p_s.at[i], p_r.at[i])
        for n in range(RING):
            part[i, n] = (t[:, n * LANES : (n + 1) * LANES] + prem[i, n].astype(F32)).astype(BF)

    def view(h, t, start, size):
        r = pl.ds(h * two + start, size)
        return (slice(None), t, r, slice(None)) if h == 0 else (t, slice(None), r, slice(None))

    first = [x, y]
    second = [y, x]

    def hop(h, stage, step):
        return device(x_=at(x, step)) if (h == 0) == (stage == 0) else device(y_=at(y, step))

    group, piece = two // 2, two // 4

    def term(h, t, r, n):
        return part.at[view(h, t, r * group + n * piece, piece)]

    def box(ref, h, side, r, n):
        return ref.at[h, side, :, pl.ds(r * group + n * piece, piece)]

    for r in (0, 1):
        for h in (0, 1):
            for n, step in ((0, RIGHT), (1, LEFT)):
                put(
                    term(h, at(first[h], FAR), r, n), relay.at[h, r, n],
                    q_s.at[h, r, n], q_r.at[h, r, n], hop(h, 0, step),
                )
        for h in (0, 1):
            for n, step in ((0, RIGHT), (1, LEFT)):
                put(
                    term(h, at(first[h], step), r, 1 - n), box(joined, h, n, r, 1 - n),
                    j_s.at[h, r, n, 0], j_r.at[h, r, n, 0], hop(h, 0, step),
                )
    finish(EVENTS[-1], (1,))

    def deltas(i, carry):
        r = pl.multiple_of(i * block, block)
        grad = acc[pl.ds(2 * units + r, block), :]
        delta[pl.ds(r, block), :] = (grad * acc[pl.ds(r, block), :]).astype(BF)
        delta[pl.ds(units + r, block), :] = (grad * acc[pl.ds(units + r, block), :]).astype(BF)
        return carry

    lax.fori_loop(0, units // block, deltas, 0)

    def gradients(i, squares):
        pair = [2 * i, 2 * i + 1]
        cols = pl.ds(pl.multiple_of(i * 2 * LANES, 2 * LANES), 2 * LANES)
        xs = jnp.concatenate([slots[0, s] for s in pair], axis=1)
        gs = jnp.concatenate([slots[1, s] for s in pair], axis=1)
        g = dot(delta[...], xs, ((1,), (0,)))
        grads[pl.ds(0, 2 * units), cols] = g
        squares += jnp.sum((g * g).reshape(2 * units // 8, 8, 2 * LANES), axis=0)
        g = dot(hid_t[pl.ds(0, units), :], gs, ((1,), (0,)))
        grads[pl.ds(2 * units, units), cols] = g
        return squares + jnp.sum((g * g).reshape(units // 8, 8, 2 * LANES), axis=0)

    def pass_terms(r):
        for h in (0, 1):
            for n, step in ((0, RIGHT), (1, LEFT)):
                arrived(relay.at[h, r, n], q_s.at[h, r, n], q_r.at[h, r, n])
                ref = term(h, at(first[h], step), r, n)
                ref[...] = (ref[...].astype(F32) + relay[h, r, n].astype(F32)).astype(BF)
                put(ref, box(joined, h, n, r, n), j_s.at[h, r, n, 1], j_r.at[h, r, n, 1], hop(h, 0, step))

    def across(r):
        for h in (0, 1):
            for n in (0, 1):
                arrived(box(joined, h, n, r, 1 - n), j_s.at[h, r, n, 0], j_r.at[h, r, n, 0])
                arrived(box(joined, h, n, r, n), j_s.at[h, r, n, 1], j_r.at[h, r, n, 1])
            v = pl.ds(r * group, group)
            half[h, :, v, :] = (
                part[view(h, first[h], r * group, group)].astype(F32)
                + joined[h, 0, :, v, :].astype(F32) + joined[h, 1, :, v, :].astype(F32)
            ).astype(BF)
            for j in (1, 2, 3):
                put(
                    half.at[h, at(second[h], j), v], last.at[h, j - 1, v],
                    l_s.at[h, r, j - 1], l_r.at[h, r, j - 1], hop(h, 1, j),
                )

    blocks = experts // 4
    place_of = (z % (2 * blocks)) // blocks * 2 * blocks + z // (2 * blocks) * blocks + z % blocks

    def give_back(r):
        for h in (0, 1):
            v = pl.ds(r * group, group)
            summed = half[h, second[h], v, :].astype(F32)
            for j in (1, 2, 3):
                arrived(last.at[h, j - 1, v], l_s.at[h, r, j - 1], l_r.at[h, r, j - 1])
                summed = summed + last[h, j - 1, v, :].astype(F32)
            final[pl.ds(h * two + r * group, group), :] = summed.astype(BF)
        for n in range(2 * blocks - 1) if r == 0 else range(2 * blocks - 1, experts - 1):
            i = n + jnp.where(n >= place_of, 1, 0)
            to = (i // blocks) % 2 * 2 * blocks + i // (2 * blocks) * blocks + i % blocks
            to_rows = pl.ds(pl.multiple_of(to * cap, cap), cap)
            put(final.at[to_rows], back.at[own_rows], k_s.at[n], k_r.at[z], device(z_=to))

    def share(stage, value, devices, base):
        sq_send[stage] = value
        for n, dev in enumerate(devices):
            put(sq_send.at[stage], sq_recv.at[base + n], sq_s.at[base + n], sq_r.at[base + n], dev)

    def gathered(value, base, n):
        for i in range(base, base + n):
            arrived(sq_recv.at[i], sq_s.at[i], sq_r.at[i])
            value = value + sq_recv[i]
        return value

    pairs = slots.shape[1] // 2
    squares = lax.fori_loop(0, 3 * pairs // 4, gradients, jnp.zeros((8, 2 * LANES), F32))
    pass_terms(0)
    squares = lax.fori_loop(3 * pairs // 4, pairs, gradients, squares)
    value = squares[:, :LANES] + squares[:, LANES:]
    share(0, value, [device(c_=1 - c)], 0)
    value = gathered(value, 0, 1)
    share(1, value, [device(x_=at(x, s)) for s in (1, 2, 3)], 1)
    pass_terms(1)
    across(0)
    value = gathered(value, 1, 3)
    share(2, value, [device(y_=at(y, s)) for s in (1, 2, 3)], 4)
    across(1)
    value = gathered(value, 4, 3)
    share(3, value, [device(z_=(z + j) % experts) for j in range(1, experts)], 7)
    give_back(0)
    give_back(1)
    back[own_rows, :] = final[own_rows, :]
    value = gathered(value, 7, experts - 1)
    inv = lax.rsqrt(jnp.sum(value, keepdims=True) / total + 1e-06)

    def scale(i, carry):
        r = pl.ds(pl.multiple_of(i * block, block), block)
        scaled_out[r, :] = (grads[r, :] * inv).astype(BF)
        return carry

    lax.fori_loop(0, 3 * units // block, scale, 0)
    for copy in started:
        copy.wait_send()
    for j in range(1, experts):
        source = (z + experts - j) % experts
        from_rows = pl.ds(pl.multiple_of(source * cap, cap), cap)
        arrived(back.at[from_rows], k_s.at[0], k_r.at[source])


def copy_body(scaled, back, hot_t, weights, gate_out, up_out, down_out, layer_out, sems):
    units = gate_out.shape[0]
    blocks = units // BLOCK
    copies = [
        pltpu.make_async_copy(
            scaled.at[pl.ds(n * units + i * BLOCK, BLOCK)], out.at[pl.ds(i * BLOCK, BLOCK)], sems.at[n * blocks + i]
        )
        for i in range(blocks) for n, out in enumerate((gate_out, up_out, down_out))
    ]
    for copy in copies:
        copy.start()
    picked = [dot(hot_t[k], back[...], ((1,), (0,))) for k in (0, 1)]
    layer_out[...] = (weights[0] * picked[0] + weights[1] * picked[1]).astype(BF)
    for copy in copies:
        copy.wait()


def solution(mesh):
    experts = mesh.shape["expert"]
    groups = mesh.shape["dp"] * mesh.shape["ffn"]

    def on_device(tokens, expert_ids, route_weight, cotangent, w_gate, w_up, w_down):
        rows, features = tokens.shape
        units = w_gate.shape[1]
        padded = -(-units // LANES) * LANES
        count = experts * rows // 2
        two, four = count // 2, count // 4
        total = 3.0 * experts * units * groups * features
        vmem, anywhere = pl.BlockSpec(memory_space=pltpu.VMEM), pl.BlockSpec(memory_space=pltpu.HBM)
        dma = pltpu.SemaphoreType.DMA
        scaled, back, hot_t, weights = pl.pallas_call(
            functools.partial(body, experts=experts, total=total),
            out_shape=[
                jax.ShapeDtypeStruct((3 * units, features), BF),
                jax.ShapeDtypeStruct((count, LANES), BF),
                jax.ShapeDtypeStruct((2, rows, count), BF),
                jax.ShapeDtypeStruct((2, rows, LANES), F32),
            ],
            in_specs=[anywhere] * 7,
            out_specs=[vmem] * 4,
            scratch_shapes=[
                pltpu.VMEM((2, rows), jnp.int32),
                pltpu.VMEM((2, rows), F32),
                pltpu.VMEM((3 * units, features), F32),
                pltpu.VMEM((len(DIRECT), rows, LANES), BF),
                pltpu.VMEM((len(DIRECT), rows, LANES), BF),
                pltpu.VMEM((2, count, rows), BF),
                pltpu.VMEM((2, len(DIRECT), count, LANES), BF),
                pltpu.VMEM((2, groups, count, LANES), BF),
                pltpu.VMEM((2 * units, features), BF),
                pltpu.VMEM((padded, features), BF),
                pltpu.VMEM((3 * units, count), F32),
                pltpu.VMEM((padded, count), BF),
                pltpu.VMEM((count, padded), BF),
                pltpu.VMEM((2 * units, count), BF),
                pltpu.VMEM((RING, RING, count, LANES), BF),
                pltpu.VMEM((RING, RING, count, LANES), BF),
                pltpu.VMEM((RING, RING, count, LANES), BF),
                pltpu.VMEM((2, 2, 2, RING, four // 2, LANES), BF),
                pltpu.VMEM((2, 2, RING, two, LANES), BF),
                pltpu.VMEM((2, RING, two, LANES), BF),
                pltpu.VMEM((2, 3, two, LANES), BF),
                pltpu.VMEM((count, LANES), BF),
                pltpu.VMEM((4, 8, LANES), F32),
                pltpu.VMEM((6 + experts, 8, LANES), F32),
                dma((11,)),
                dma((2, len(DIRECT), experts - 1)), dma((2, len(DIRECT), experts - 1)),
                dma((2, 4)), dma((2, 4)),
                dma((2, RING, 4)), dma((2, RING, 4)),
                dma((2, RING, RING)), dma((2, RING, RING)),
                dma((RING,)), dma((RING,)),
                dma((2, 2, 2)), dma((2, 2, 2)),
                dma((2, 2, 2, 2)), dma((2, 2, 2, 2)),
                dma((2, 2, 3)), dma((2, 2, 3)),
                dma((experts - 1,)), dma((experts,)),
                dma((6 + experts,)), dma((6 + experts,)),
            ],
            compiler_params=pltpu.CompilerParams(
                collective_id=0, has_side_effects=True, vmem_limit_bytes=VMEM
            ),
            name="layer",
        )(
            *[
                pltpu.with_memory_space_constraint(a, pltpu.HBM)
                for a in (expert_ids.T, route_weight.T, tokens, cotangent, w_gate, w_up, w_down)
            ]
        )
        gate, up, down, layer = pl.pallas_call(
            copy_body,
            out_shape=[jax.ShapeDtypeStruct((units, features), BF)] * 3
            + [jax.ShapeDtypeStruct((rows, LANES), BF)],
            in_specs=[vmem] * 4,
            out_specs=[anywhere] * 3 + [vmem],
            scratch_shapes=[dma((3 * (units // BLOCK),))],
            compiler_params=pltpu.CompilerParams(vmem_limit_bytes=COPY_VMEM),
            name="copy_out",
        )(scaled, back, hot_t, weights)
        return layer, gate[None], up[None], down[None]

    token, hidden = P("expert", None), P("expert", ("dp", "ffn"), None)
    return jax.shard_map(
        on_device,
        mesh=mesh,
        in_specs=(token, token, token, token, hidden, hidden, hidden),
        out_specs=(P("expert", ("dp", "ffn")), hidden, hidden, hidden),
        check_vma=False,
    )
```
